32 devices in a mesh: py: 8 (over y, x, core), pz: 4 (over z).
Axes of the slice: x: 2, y: 2, z: 4, core: 2. Of those that a mesh axis runs over, the one named last changes fastest.
Arguments:
- velocity: float32 [3, 8, 1024, 1024], P(None, 'py', 'pz'), may hold values from -14 to 14
Outputs:
- nu_t: float32 [8, 1024, 1024], P('py', 'pz')
- filtered_velocity: bfloat16 [3, 8, 1024, 1024], P(None, 'py', None, 'pz')
The draws below stay inside these ranges and needn't reach their ends.
All inputs are finite; a program needn't handle non-finite values.
Results may differ from the reference program's by a relative error of at most 0.012.
The reference program's roundings to bfloat16 on the way count: a program that leaves them out, or rounds other values in their place, can miss the bound.
Values may be sent and summed in bfloat16 or wider, within the bound.
A program may use at most 64 MiB of HBM per device.

```python
import math
import jax
import jax.numpy as jnp
import numpy as np
from jax import lax

NX = 1024
NZ = 1024
NY = 8


def draw_velocity(key, part):
    base = jax.random.fold_in(key, 17)
    noise_key, span_key, stream_key = jax.random.split(base, 3)
    heights = (jnp.arange(NY, dtype=jnp.float32) + 0.5) * (2.0 / NY) - 1.0
    profile = 1.5 * (1.0 - heights * heights)
    offset = jnp.stack([profile, jnp.zeros_like(profile), jnp.zeros_like(profile)])[:, :, None, None]
    span_frac = jnp.arange(NZ, dtype=jnp.float32) / NZ
    span_scale = jnp.exp(jnp.log(3.0) * span_frac + jax.random.uniform(span_key, (NZ,), jnp.float32, 0.0, jnp.log(1.8)))
    stream_scale = jnp.exp(jax.random.uniform(stream_key, (NX,), jnp.float32, 0.0, jnp.log(1.8)))
    amplitude = 0.25 * span_scale[:, None] * stream_scale[None, :]
    values = jnp.clip(jax.random.normal(noise_key, (3, NY, NZ, NX), jnp.float32), -5.0, 5.0) * amplitude
    return values + offset


def setup_inputs(seed: int = 0) -> dict:
    splits = jax.random.split(jax.random.key(seed), 2)
    return {
        "velocity": draw_velocity(jax.random.fold_in(splits[1], 71), 0),
    }


index_pairs = ((0, 0), (1, 1), (2, 2), (0, 1), (0, 2), (1, 2))
pair_weights = (1.0, 1.0, 1.0, 2.0, 2.0, 2.0)
epsilon = 1e-06

def filter_table(length):
    offsets = np.arange(length, dtype=np.int64)
    wavenumbers = np.arange(1, length // 4, dtype=np.int64)
    phase = offsets[:, None] * wavenumbers[None, :] % length
    kernel = (1.0 + 2.0 * np.cos(phase * (2.0 * math.pi / length)).sum(axis=1)) / length
    kernel = kernel.astype(np.float32)
    lagged = (offsets[:, None] - offsets[None, :]) % length
    return jnp.asarray(kernel[lagged], dtype=jnp.float32).astype(jnp.bfloat16)

def smooth_fields(fields, table_x, table_z):
    fields = lax.optimization_barrier(fields)
    along_x = jnp.einsum('fzx,xv->fzv', fields.astype(jnp.float32), table_x.astype(jnp.float32), precision=lax.Precision.HIGHEST).astype(jnp.bfloat16)
    along_x = lax.optimization_barrier(along_x)
    return jnp.einsum('wz,fzx->fwx', table_z.astype(jnp.float32), along_x.astype(jnp.float32), precision=lax.Precision.HIGHEST).astype(jnp.bfloat16)

def row_slopes(rows):
    rows = rows.astype(jnp.float32)
    center = rows[:, 1]
    slope_x = (jnp.roll(center, -1, 2) - jnp.roll(center, 1, 2)) * 0.5
    slope_z = (jnp.roll(center, -1, 1) - jnp.roll(center, 1, 1)) * 0.5
    slope_y = (rows[:, 2] - rows[:, 0]) * 0.5
    return (slope_x, slope_y, slope_z)

def strain(gradients):
    strain_parts = [0.5 * (gradients[b][a] + gradients[a][b]) for a, b in index_pairs]
    squares_sum = pair_weights[0] * strain_parts[0] * strain_parts[0]
    for weight, part_value in zip(pair_weights[1:], strain_parts[1:]):
        squares_sum = squares_sum + weight * part_value * part_value
    return (strain_parts, jnp.sqrt(2.0 * squares_sum))

def reference(velocity):
    table_x = filter_table(NX)
    table_z = filter_table(NZ)
    wall_rows = jnp.zeros((3, 1, NZ, NX), velocity.dtype)
    velocity_padded = jnp.concatenate([wall_rows, velocity, wall_rows], axis=1)

    def first_pass(row):
        center = lax.dynamic_slice_in_dim(velocity, row, 1, 1)[:, 0]
        return smooth_fields(center.astype(jnp.bfloat16), table_x, table_z)
    filtered_rows = lax.map(first_pass, jnp.arange(NY, dtype=jnp.int32))
    filtered_velocity = jnp.transpose(filtered_rows, (1, 0, 2, 3))
    wall_filtered = jnp.zeros((3, 1, NZ, NX), filtered_velocity.dtype)
    filtered_padded = jnp.concatenate([wall_filtered, filtered_velocity, wall_filtered], axis=1)

    def second_pass(row):
        rows_velocity = lax.dynamic_slice_in_dim(velocity_padded, row, 3, 1)
        rows_filtered = lax.dynamic_slice_in_dim(filtered_padded, row, 3, 1).astype(jnp.float32)
        strain_parts, magnitude = strain(row_slopes(rows_velocity))
        center = rows_velocity[:, 1]
        pieces = [(center[a] * center[b]).astype(jnp.bfloat16) for a, b in index_pairs]
        pieces = pieces + [(magnitude * part_value).astype(jnp.bfloat16) for part_value in strain_parts]
        smoothed = smooth_fields(jnp.stack(pieces), table_x, table_z).astype(jnp.float32)
        hat_parts, magnitude_hat = strain(row_slopes(rows_filtered))
        smooth_velocity = rows_filtered[:, 1]
        numerator = jnp.zeros_like(magnitude)
        denominator = jnp.zeros_like(magnitude)
        for pair_index, (a, b) in enumerate(index_pairs):
            leonard = smoothed[pair_index] - smooth_velocity[a] * smooth_velocity[b]
            model_term = smoothed[6 + pair_index] - 4.0 * magnitude_hat * hat_parts[pair_index]
            numerator = numerator + pair_weights[pair_index] * leonard * model_term
            denominator = denominator + pair_weights[pair_index] * model_term * model_term
        return (jnp.sum(numerator), jnp.sum(denominator), magnitude)
    numerator, denominator, magnitude = lax.map(second_pass, jnp.arange(NY, dtype=jnp.int32))
    plane_cells = NX * NZ
    coefficient = numerator / plane_cells / (2.0 * (denominator / plane_cells + epsilon))
    nu_t = coefficient[:, None, None] * magnitude
    return (nu_t, filtered_velocity)
```

```python
import functools
import math

import jax
import jax.numpy as jnp
import numpy as np
from jax import lax
from jax.experimental import pallas as pl
from jax.experimental.pallas import tpu as pltpu
from jax.sharding import PartitionSpec as P

index_pairs = ((0, 0), (1, 1), (2, 2), (0, 1), (0, 2), (1, 2))
pair_weights = (1.0, 1.0, 1.0, 2.0, 2.0, 2.0)
epsilon = 1e-06


def neighbours(first, last, axis, wrap):
    n = lax.axis_size(axis)
    up = [(i, (i + 1) % n) for i in range(n) if wrap or i + 1 < n]
    down = [(j, i) for i, j in up]
    return lax.ppermute(last, axis, up), lax.ppermute(first, axis, down)


def filter_taps(length):
    offsets = np.arange(length, dtype=np.int64)
    wavenumbers = np.arange(1, length // 4, dtype=np.int64)
    phase = offsets[:, None] * wavenumbers[None, :] % length
    kernel = (1.0 + 2.0 * np.cos(phase * (2.0 * math.pi / length)).sum(axis=1)) / length
    return kernel.astype(np.float32)


def filter_table(length):
    offsets = np.arange(length, dtype=np.int64)
    lagged = (offsets[:, None] - offsets[None, :]) % length
    return jnp.asarray(filter_taps(length)[lagged], dtype=jnp.float32).astype(jnp.bfloat16)


def strain(gradients):
    strain_parts = [0.5 * (gradients[b][a] + gradients[a][b]) for a, b in index_pairs]
    squares_sum = pair_weights[0] * strain_parts[0] * strain_parts[0]
    for weight, part_value in zip(pair_weights[1:], strain_parts[1:]):
        squares_sum = squares_sum + weight * part_value * part_value
    return strain_parts, jnp.sqrt(2.0 * squares_sum)


def filter_z_kernel(n, *refs):
    table, blocks, out = refs[0], refs[1 : 1 + n], refs[1 + n]
    width = blocks[0].shape[1]
    rows = min(512, out.shape[1])
    for top in range(0, out.shape[1], rows):
        total = None
        for s in range(n):
            term = jnp.dot(
                table[top : top + rows, s * width : (s + 1) * width],
                blocks[s][0],
                preferred_element_type=jnp.float32,
            )
            total = term if total is None else total + term
        out[0, top : top + rows, :] = total.astype(out.dtype)


def filter_z(table, blocks):
    n, (fields, width, columns) = len(blocks), blocks[0].shape
    length = table.shape[0]
    return pl.pallas_call(
        functools.partial(filter_z_kernel, n),
        grid=(fields,),
        in_specs=[pl.BlockSpec(table.shape, lambda f: (0, 0), pipeline_mode=pl.Buffered(1))]
        + [pl.BlockSpec((1, width, columns), lambda f: (f, 0, 0))] * n,
        out_specs=pl.BlockSpec((1, length, columns), lambda f: (f, 0, 0)),
        out_shape=jax.ShapeDtypeStruct((fields, length, columns), jnp.bfloat16),
        cost_estimate=pl.CostEstimate(
            flops=2 * fields * length * length * columns,
            bytes_accessed=4 * fields * length * columns + 2 * length * length,
            transcendentals=0,
        ),
    )(table, *blocks)


def coarse_kernel(hat, below, above, before, after, out, u):
    length, columns = hat.shape[1:]
    rows = min(64, length)
    for a in range(3):
        u[a, 8 : 8 + length, :] = hat[a].astype(jnp.float32)
        u[a, 0:8, :] = hat[a, length - 16 : length, :].astype(jnp.float32)[8:]
        u[a, 8 + length : 16 + length, :] = hat[a, 0:16, :].astype(jnp.float32)[:8]
    lane = lax.broadcasted_iota(jnp.int32, (rows, columns), 1)

    def tile(i, carry):
        top = pl.multiple_of(i * rows, rows)
        here = pl.ds(top, rows)
        grad = []
        for a in range(3):
            around = u[a, pl.ds(top, rows + 16), :]
            centre = around[8 : 8 + rows]
            left, right = pltpu.roll(centre, 1, 1), pltpu.roll(centre, columns - 1, 1)
            left = jnp.where(lane == 0, before[a, here, :].astype(jnp.float32), left)
            right = jnp.where(lane == columns - 1, after[a, here, :].astype(jnp.float32), right)
            slope_y = above[a, here, :].astype(jnp.float32) - below[a, here, :].astype(jnp.float32)
            slope_z = around[9 : 9 + rows] - around[7 : 7 + rows]
            grad.append([(right - left) * 0.5, slope_y * 0.5, slope_z * 0.5])
        parts, magnitude = strain(grad)
        for p, part in enumerate(parts):
            out[p, here, :] = 4.0 * magnitude * part
        return carry

    lax.fori_loop(0, length // rows, tile, 0)


def coarse_model(hat, below, above, before, after):
    _, length, columns = hat.shape
    vmem = pl.BlockSpec(memory_space=pltpu.VMEM)
    return pl.pallas_call(
        coarse_kernel,
        in_specs=[vmem] * 5,
        out_specs=vmem,
        out_shape=jax.ShapeDtypeStruct((6, length, columns), jnp.float32),
        scratch_shapes=[pltpu.VMEM((3, length + 16, columns), jnp.float32)],
        cost_estimate=pl.CostEstimate(
            flops=100 * length * columns, bytes_accessed=42 * length * columns, transcendentals=0
        ),
    )(hat, below, above, before, after)


def lilly_kernel(n, weight, *refs):
    table, blocks = refs[0], refs[1 : 1 + n]
    product, left, right, coarse, start, out = refs[1 + n :]
    width, columns = blocks[0].shape[1:]
    rows = min(256, product.shape[1])

    @pl.when(pl.program_id(0) == 0)
    def _():
        out[...] = start[...]

    for top in range(0, product.shape[1], rows):
        here = slice(top, top + rows)
        total = None
        for s in range(n):
            term = jnp.dot(
                table[here, s * width : (s + 1) * width],
                blocks[s][0],
                preferred_element_type=jnp.float32,
            )
            total = term if total is None else total + term
        fine = total.astype(jnp.bfloat16).astype(jnp.float32)
        model = fine - coarse[0, here, :]
        leonard = product[0, here, :].astype(jnp.float32) - left[0, here, :].astype(
            jnp.float32
        ) * right[0, here, :].astype(jnp.float32)
        for i, value in enumerate((leonard * model, model * model)):
            out[i] += weight * jnp.sum(value.reshape(rows // 8, 8, columns), axis=0)


def lilly(table, blocks, products, hat, coarse, first, start):
    n, (fields, width, columns) = len(blocks), blocks[0].shape
    length = table.shape[0]
    a0, b0 = index_pairs[first]
    a1, b1 = index_pairs[first + 1] if fields > 1 else (a0, b0)

    def plane(offset, step=1):
        return pl.BlockSpec((1, length, columns), lambda f: (offset + f * step, 0, 0))

    for f in range(fields):
        assert index_pairs[first + f] == (a0 + f * (a1 - a0), b0 + f * (b1 - b0))
        assert pair_weights[first + f] == pair_weights[first]
    sums = pl.BlockSpec(start.shape, lambda f: (0, 0, 0))
    return pl.pallas_call(
        functools.partial(lilly_kernel, n, pair_weights[first]),
        grid=(fields,),
        in_specs=[pl.BlockSpec(table.shape, lambda f: (0, 0), pipeline_mode=pl.Buffered(1))]
        + [pl.BlockSpec((1, width, columns), lambda f: (f, 0, 0))] * n
        + [plane(first), plane(a0, a1 - a0), plane(b0, b1 - b0), plane(first), sums],
        out_specs=sums,
        out_shape=jax.ShapeDtypeStruct(start.shape, jnp.float32),
        cost_estimate=pl.CostEstimate(
            flops=2 * fields * length * length * columns,
            bytes_accessed=12 * fields * length * columns + 2 * length * length,
            transcendentals=0,
        ),
    )(table, *blocks, products, hat, hat, coarse, start)


def coefficient_kernel(n, cells, part, out, held, send_sem, recv_sem):
    me = lax.axis_index("pz")
    barrier = pltpu.get_barrier_semaphore()
    others = [lax.rem(me + s, n) for s in range(1, n)]
    for other in others:
        pl.semaphore_signal(
            barrier, inc=1, device_id={"pz": other}, device_id_type=pl.DeviceIdType.MESH
        )
    pl.semaphore_wait(barrier, n - 1)
    copies = [
        pltpu.make_async_remote_copy(
            src_ref=part,
            dst_ref=held.at[s],
            send_sem=send_sem.at[s],
            recv_sem=recv_sem.at[s],
            device_id={"pz": other},
            device_id_type=pl.DeviceIdType.MESH,
        )
        for s, other in enumerate(others)
    ]
    for copy in copies:
        copy.start()
    total = part[...]
    for s, copy in enumerate(copies):
        copy.wait()
        total = total + held[s]
    mean = jnp.sum(jnp.sum(total, axis=2, keepdims=True), axis=1, keepdims=True) / cells
    value = mean[0] / (2.0 * (mean[1] + epsilon))
    out[...] = jnp.broadcast_to(value, out.shape)


def coefficient_of(part, cells, columns):
    n = lax.axis_size("pz")
    return pl.pallas_call(
        functools.partial(coefficient_kernel, n, cells),
        in_specs=[pl.BlockSpec(memory_space=pltpu.VMEM)],
        out_specs=pl.BlockSpec(memory_space=pltpu.VMEM),
        out_shape=jax.ShapeDtypeStruct((8, columns), jnp.float32),
        scratch_shapes=[
            pltpu.VMEM((n - 1,) + part.shape, jnp.float32),
            pltpu.SemaphoreType.DMA((n - 1,)),
            pltpu.SemaphoreType.DMA((n - 1,)),
        ],
        compiler_params=pltpu.CompilerParams(collective_id=0, has_side_effects=True),
    )(part)


def body(velocity):
    n, me = lax.axis_size("pz"), lax.axis_index("pz")
    v = velocity[:, 0]
    depth, nx = v.shape[1:]
    nz, width = depth * n, nx // n
    table_x = filter_table(nx)
    table_z = table_x if nz == nx else filter_table(nz)
    to_x = [
        lax.dynamic_slice_in_dim(table_x, lax.rem(me + s, n) * width, width, 1) for s in range(n)
    ]
    from_z = jnp.concatenate(
        [
            lax.dynamic_slice_in_dim(table_z, lax.rem(me - s + n, n) * depth, depth, 1)
            for s in range(n)
        ],
        axis=1,
    )
    order = list(range(n - 1, 0, -1))
    order.sort(key=lambda s: -min(s, n - s))

    def exchange(pieces):
        fields = jnp.stack([p.astype(jnp.bfloat16) for p in pieces])
        blocks = [None] * n
        for s in order + [0]:
            along = jnp.einsum(
                "fzx,xv->fzv", fields, to_x[s], preferred_element_type=jnp.float32
            ).astype(jnp.bfloat16)
            if s:
                along = lax.ppermute(along, "pz", [(i, (i + s) % n) for i in range(n)])
            blocks[s] = along
        return blocks

    blocks_v = exchange([v[a] for a in range(3)])
    below, above = neighbours(v, v, "py", False)
    before, after = neighbours(v[:, :1], v[:, -1:], "pz", True)
    blocks_p = exchange([v[a] * v[b] for a, b in index_pairs])

    padded = jnp.concatenate([before, v, after], axis=1)
    slope_x = (jnp.roll(v, -1, 2) - jnp.roll(v, 1, 2)) * 0.5
    slope_y = (above - below) * 0.5
    slope_z = (padded[:, 2:] - padded[:, :-2]) * 0.5
    grad = [[slope_x[a], slope_y[a], slope_z[a]] for a in range(3)]
    parts, magnitude = strain([[g[b] for b in range(3)] for g in grad])
    groups = ((0, 3), (3, 5), (5, 6))
    blocks_s = [
        exchange([magnitude * part for part in parts[first:last]]) for first, last in groups
    ]
    from_z, *local = lax.optimization_barrier((from_z, *[blocks[0] for blocks in blocks_s]))
    for blocks, own in zip(blocks_s, local):
        blocks[0] = own

    hat = filter_z(from_z, blocks_v)
    below, above = neighbours(hat, hat, "py", False)
    before, after = neighbours(hat[:, :, :1], hat[:, :, -1:], "pz", True)
    coarse = coarse_model(hat, below, above, before, after)
    products = filter_z(from_z, blocks_p)
    sums = jnp.zeros((2, 8, width), jnp.float32)
    for (first, _), blocks in zip(groups, blocks_s):
        sums = lilly(from_z, blocks, products, hat, coarse, first, sums)
    coefficient = coefficient_of(sums, nx * nz, nx)
    nu_t = magnitude.reshape(depth // 8, 8, nx) * coefficient
    return nu_t.reshape(1, depth, nx), hat[:, None]


MESH = pl.DeviceIdType.MESH


def round_up(value, step):
    return -(-value // step) * step


def cross_factors(length, width, offset):
    taps = filter_taps(length).astype(jnp.bfloat16).astype(np.float64)
    cells = np.arange(width)
    block = taps[(offset * width + cells[:, None] - cells[None, :]) % length]
    _, values, rows = np.linalg.svd(block)
    basis = rows[: int((values > 1e-3).sum())]
    probe = np.cos(0.37 * cells) + cells / width
    basis = basis * np.where(basis @ probe < 0, -1.0, 1.0)[:, None]
    basis = basis.astype(jnp.bfloat16).astype(np.float64)
    return np.linalg.lstsq(basis.T, block.T, rcond=None)[0].T, basis


def cross_tables(factors, fields, width):
    spans, top = {}, 0
    for s, (a, b) in factors.items():
        spans[s] = (top, round_up(fields * b.shape[0], 16))
        top += spans[s][1]
    down = np.zeros((top, fields * width))
    back = np.zeros((fields, width, top))
    for s, (a, b) in factors.items():
        rank = b.shape[0]
        for f in range(fields):
            rows = slice(spans[s][0] + f * rank, spans[s][0] + (f + 1) * rank)
            down[rows, f * width : (f + 1) * width] = b
            back[f][:, rows] = a
    return (
        jnp.asarray(down.astype(np.float32), dtype=jnp.bfloat16),
        jnp.asarray(back.astype(np.float32), dtype=jnp.bfloat16),
        spans,
    )


def plane_kernel(n, ny, spans_v, spans_p, *refs):
    velocity, table, near, down_v, back_v, down_p, back_p, nu, hat = refs[:9]
    v, below, above, detoured, u, hat_z = refs[9:15]
    along_v, along, along_y, x, scaled, product, coarse, fine = refs[15:23]
    edge_out, edge_in, hat_edge_out, hat_edge_in = refs[23:27]
    sent_v, held_v, held_below, held_above, sent_p, held_p, sent_s, held_s = refs[27:35]
    sums, sums_out, sums_in = refs[35:38]
    load_sem, edge_send, edge_recv, halo_send, halo_recv, detour_recv, onward_send = refs[38:45]
    cross_send, cross_recv, hat_send, hat_recv, pass_send, pass_recv, sum_send, sum_recv = refs[45:]

    iy, iz = lax.axis_index("py"), lax.axis_index("pz")
    depth, nx = nu.shape
    width = nx // n
    quarter = depth // 4
    half = quarter // 2
    middle = ny // 2
    detours = ny == 8
    tile = 256
    columns = [slice(left, left + tile) for left in range(0, nx, tile)]
    f32, bf16 = jnp.float32, jnp.bfloat16

    def remote(src, dst, send, recv, **device):
        return pltpu.make_async_remote_copy(
            src_ref=src,
            dst_ref=dst,
            send_sem=send,
            recv_sem=recv,
            device_id=device,
            device_id_type=MESH,
        )

    def dot(a, b):
        return jnp.dot(a, b, preferred_element_type=f32)

    def ring(s):
        return lax.rem(iz + s, n)

    loads = [
        pltpu.make_async_copy(velocity.at[a], v.at[a, 8 : 8 + depth], load_sem.at[a])
        for a in range(3)
    ]
    for load in loads:
        load.start()
    barrier = pltpu.get_barrier_semaphore()
    for s in range(1, n):
        pl.semaphore_signal(barrier, inc=1, device_id={"pz": ring(s)}, device_id_type=MESH)
    for s in range(1, ny):
        pl.semaphore_signal(
            barrier, inc=1, device_id={"py": lax.rem(iy + s, ny)}, device_id_type=MESH
        )
    pl.semaphore_wait(barrier, n - 1 + ny - 1)
    for load in loads:
        load.wait()

    def halo(way, c, h):
        row = c * quarter + h * half
        return remote(
            v.at[:, pl.ds(pl.multiple_of(8 + row, 8), half)],
            (below, above)[way].at[:, pl.ds(pl.multiple_of(row, 8), half)],
            halo_send.at[way, c, h],
            halo_recv.at[way, c, h],
            py=iy + (1, -1)[way],
        )

    def detour(way, c):
        return remote(
            v.at[:, pl.ds(8 + c * quarter + half, half)],
            detoured.at[:, pl.ds(c * half, half)],
            halo_send.at[way, c, 1],
            detour_recv.at[c],
            py=iy + (middle, -middle)[way],
        )

    def onward(way, c):
        return remote(
            detoured.at[:, pl.ds(c * half, half)],
            (below, above)[way].at[:, pl.ds(c * quarter + half, half)],
            onward_send.at[c],
            halo_recv.at[way, c, 1],
            py=iy + (1 - middle, middle - 1)[way],
        )

    has_next = (iy < ny - 1, iy > 0)
    has_last = (iy > 0, iy < ny - 1)
    bridge = (iy == middle - 1, iy == middle)
    relay = (iy == ny - 1, iy == 0)

    for way in range(2):

        @pl.when(has_next[way])
        def _(way=way):
            for c in range(4):
                halo(way, c, 0).start()
                if detours:

                    @pl.when(bridge[way])
                    def _(way=way, c=c):
                        detour(way, c).start()

                    @pl.when(jnp.logical_not(bridge[way]))
                    def _(way=way, c=c):
                        halo(way, c, 1).start()

                else:
                    halo(way, c, 1).start()

    def pass_on(c):
        if detours:
            for way in range(2):

                @pl.when(relay[way])
                def _(way=way):
                    detour(way, c).wait_recv()
                    onward(way, c).start()

    def edges(source, out, into, which):
        for a in range(3):
            out[0, a : a + 1, :] = source[a, 7 + depth : 8 + depth, :]
            out[1, a : a + 1, :] = source[a, 8:9, :]
        return [
            remote(
                out.at[side],
                into.at[side],
                edge_send.at[which, side],
                edge_recv.at[which, side],
                pz=ring((1, n - 1)[side]),
            )
            for side in range(2)
        ]

    def fill_edges(into, target):
        for a in range(3):
            target[a, 7:8, :] = into[0, a : a + 1, :]
            target[a, 8 + depth : 9 + depth, :] = into[1, a : a + 1, :]

    rims = edges(v, edge_out, edge_in, 0)
    for rim in rims:
        rim.start()

    for empty, (rows, held) in enumerate(((below, held_below), (above, held_above))):

        @pl.when(jnp.logical_not(has_last[empty]))
        def _(rows=rows, held=held):
            held[...] = jnp.zeros_like(held)

            def clear(i, carry):
                rows[:, pl.ds(pl.multiple_of(i * 8, 8), 8)] = jnp.zeros((3, 8, nx), f32)
                return carry

            lax.fori_loop(0, depth // 8, clear, 0)

    def along_x(dst, f, a, b):
        def convert(i, carry):
            row = pl.multiple_of(i * 32, 32)
            value = v[a, pl.ds(8 + row, 32)]
            if b is not None:
                value = value * v[b, pl.ds(8 + row, 32)]
            x[pl.ds(row, 32)] = value.astype(bf16)
            return carry

        lax.fori_loop(0, depth // 32, convert, 0)
        top = pl.multiple_of(f * depth, depth)
        for cols in columns:
            dst[pl.ds(top, depth), cols] = dot(x[0:depth], table[:, cols]).astype(bf16)

    def loop(count, step):
        lax.fori_loop(0, count, lambda i, carry: (step(i), carry)[1], 0)

    def cross(down, source, out, held, spans, group):
        for cols in columns:
            out[:, cols] = dot(down[...], source[:, cols]).astype(bf16)
        return [
            remote(
                out.at[top : top + rows],
                held.at[top : top + rows],
                cross_send.at[group, s - 1],
                cross_recv.at[group, s - 1],
                pz=ring(s),
            )
            for s, (top, rows) in spans.items()
        ]

    def along_z(source, f, back, held, cols):
        top = pl.multiple_of(f * depth, depth)
        return dot(near[...], source[pl.ds(top, depth), cols]) + dot(back[f], held[:, cols])

    loop(3, lambda a: along_x(along_v, a, a, None))
    out_v = cross(down_v, along_v, sent_v, held_v, spans_v, 0)
    for copy in out_v:
        copy.start()
    pass_on(0)
    loop(3, lambda i: along_x(along, i, i, i))
    pass_on(1)
    loop(2, lambda i: along_x(along, i + 3, 0, i + 1))
    along_x(along, 5, 1, 2)
    out_p = cross(down_p, along, sent_p, held_p, spans_p, 1)
    for copy in out_p:
        copy.start()
    pass_on(2)

    for copy in out_v:
        copy.wait_recv()
    passes = [
        remote(held_v, (held_below, held_above)[way], pass_send.at[way], pass_recv.at[way],
               py=iy + (1, -1)[way])
        for way in range(2)
    ]
    for way in range(2):

        @pl.when(has_next[way])
        def _(way=way):
            passes[way].start()

    def smooth_velocity(a):
        for cols in columns:
            value = along_z(along_v, a, back_v, held_v, cols).astype(bf16)
            hat_z[a, :, cols] = value
            u[a, 8 : 8 + depth, cols] = value.astype(f32)

    loop(3, smooth_velocity)
    hat_rims = edges(u, hat_edge_out, hat_edge_in, 1)
    for rim in hat_rims:
        rim.start()

    def range_of(index):
        return pl.ds(pl.multiple_of(index * width, 128), width)

    mine = pl.ds(pl.multiple_of(iz * depth, depth), depth)
    turns = [
        remote(
            hat_z.at[:, :, range_of(ring(s))],
            hat.at[:, mine],
            hat_send.at[s - 1],
            hat_recv.at[s - 1],
            pz=ring(s),
        )
        for s in (2, 1, 3)
    ]
    for turn in turns:
        turn.start()
    for a in range(3):
        hat[a, mine, :] = hat_z[a, :, range_of(iz)]
    pass_on(3)

    for copy in out_p:
        copy.wait_recv()

    def smooth_product(p):
        for cols in columns:
            product[p, :, cols] = along_z(along, p, back_p, held_p, cols).astype(bf16)

    loop(6, smooth_product)

    for rim in rims:
        rim.wait_recv()
    fill_edges(edge_in, v)

    def strain_rows(source, lower, upper, row):
        grad = []
        here = pl.ds(row, 8)
        for a in range(3):
            around = source[a, pl.ds(row, 24)]
            centre = around[8:16]
            slope_x = pltpu.roll(centre, nx - 1, 1) - pltpu.roll(centre, 1, 1)
            slope_y = upper[a, here] - lower[a, here]
            slope_z = around[9:17] - around[7:15]
            grad.append([slope_x * 0.5, slope_y * 0.5, slope_z * 0.5])
        return strain(grad)

    def chunk(c):
        for way in range(2):

            @pl.when(has_last[way])
            def _(way=way):
                halo(way, c, 0).wait_recv()
                halo(way, c, 1).wait_recv()

        base = pl.multiple_of(c * quarter, quarter)

        def strain_tile(i):
            row = pl.multiple_of(base + i * 8, 8)
            parts, magnitude = strain_rows(v, below, above, row)
            nu[pl.ds(row, 8)] = magnitude
            for p in range(6):
                scaled[p, pl.ds(pl.multiple_of(i * 8, 8), 8)] = magnitude * parts[p]

        loop(quarter // 8, strain_tile)

        def project(pick, dst):
            def convert(p):
                x[pl.ds(pl.multiple_of(p * quarter, quarter), quarter)] = pick(p).astype(bf16)

            if isinstance(pick, list):
                for p, rows in enumerate(pick):
                    top = p * quarter
                    x[top : top + quarter] = rows[0][rows[1], pl.ds(base, quarter)].astype(bf16)
            else:
                loop(6, convert)
            for cols in columns:
                value = dot(x[0 : 6 * quarter], table[:, cols]).astype(bf16)
                for p in range(6):
                    dst[pl.ds(pl.multiple_of(p * depth + base, quarter), quarter), cols] = value[
                        p * quarter : (p + 1) * quarter
                    ]

        project(lambda p: scaled[p], along)
        project([(rows, a) for rows in (below, above) for a in range(3)], along_y)

    loop(4, chunk)
    out_s = cross(down_p, along, sent_s, held_s, spans_p, 2)
    for copy in out_s:
        copy.start()

    for way, (rows, held) in enumerate(((below, held_below), (above, held_above))):

        @pl.when(has_last[way])
        def _(way=way):
            passes[way].wait_recv()

        def smooth_rows(a, way=way, rows=rows, held=held):
            for cols in columns:
                value = (
                    dot(near[...], along_y[pl.ds(pl.multiple_of((way * 3 + a) * depth, depth), depth), cols])
                    + dot(back_v[a], held[:, cols])
                )
                rows[a, :, cols] = value.astype(bf16).astype(f32)

        loop(3, smooth_rows)

    for rim in hat_rims:
        rim.wait_recv()
    fill_edges(hat_edge_in, u)

    def coarse_tile(i):
        row = pl.multiple_of(i * 8, 8)
        parts, magnitude = strain_rows(u, below, above, row)
        for p in range(6):
            coarse[p, pl.ds(row, 8)] = 4.0 * magnitude * parts[p]

    loop(depth // 8, coarse_tile)

    for copy in out_s:
        copy.wait_recv()
    sums[...] = jnp.zeros_like(sums)
    for p, (a, b) in enumerate(index_pairs):
        for cols in columns:
            value = along_z(along, p, back_p, held_s, cols)
            fine[:, cols] = value.astype(bf16).astype(f32)

        def lilly_tile(i, total, p=p, a=a, b=b):
            row = pl.multiple_of(i * 16, 16)
            here, there = pl.ds(row, 16), pl.ds(8 + row, 16)
            model = fine[here] - coarse[p, here]
            leonard = product[p, here].astype(f32) - u[a, there] * u[b, there]
            numerator, denominator = leonard * model, model * model
            return (
                total[0] + numerator[0:8] + numerator[8:16],
                total[1] + denominator[0:8] + denominator[8:16],
            )

        zero = jnp.zeros((8, nx), f32)
        totals = lax.fori_loop(0, depth // 16, lilly_tile, (zero, zero))
        for i in range(2):
            sums[i] += pair_weights[p] * totals[i]

    for i in range(2):
        value = sums[i]
        part = value[:, 0:128]
        for left in range(128, nx, 128):
            part = part + value[:, left : left + 128]
        sums_out[i] = part
    shares = [
        remote(sums_out, sums_in.at[s - 1], sum_send.at[s - 1], sum_recv.at[s - 1], pz=ring(s))
        for s in range(1, n)
    ]
    for share in shares:
        share.start()
    total = sums_out[...]
    for s, share in enumerate(shares):
        share.wait_recv()
        total = total + sums_in[s]
    cells = float(nx * depth * n)
    mean = jnp.sum(jnp.sum(total, axis=2, keepdims=True), axis=1, keepdims=True) / cells
    coefficient = jnp.broadcast_to(mean[0] / (2.0 * (mean[1] + epsilon)), (8, nx))

    def scale(i):
        here = pl.ds(pl.multiple_of(i * 8, 8), 8)
        nu[here] = nu[here] * coefficient

    loop(depth // 8, scale)

    for turn in turns:
        turn.wait_recv()
    for copy in rims + hat_rims + out_v + out_p + out_s + turns + shares:
        copy.wait_send()
    for way in range(2):

        @pl.when(has_next[way])
        def _(way=way):
            passes[way].wait_send()
            for c in range(4):
                halo(way, c, 0).wait_send()
                halo(way, c, 1).wait_send()

        if detours:

            @pl.when(relay[way])
            def _(way=way):
                for c in range(4):
                    onward(way, c).wait_send()


def plane_body(velocity):
    n, ny = lax.axis_size("pz"), lax.axis_size("py")
    depth, nx = velocity.shape[2:]
    nz, width, quarter = depth * n, nx // n, depth // 4
    factors = {s: cross_factors(nz, depth, s) for s in (1, n - 1, 2)}
    down_v, back_v, spans_v = cross_tables(factors, 3, depth)
    down_p, back_p, spans_p = cross_tables(factors, 6, depth)
    cells = np.arange(depth)
    near = filter_taps(nz)[(cells[:, None] - cells[None, :]) % nz]
    near = jnp.asarray(near, dtype=jnp.float32).astype(jnp.bfloat16)
    f32, bf16 = jnp.float32, jnp.bfloat16
    vmem = pl.BlockSpec(memory_space=pltpu.VMEM)
    dma = pltpu.SemaphoreType.DMA
    rows_v, rows_p = down_v.shape[0], down_p.shape[0]
    scratch = [
        pltpu.VMEM((3, depth + 16, nx), f32),
        pltpu.VMEM((3, depth, nx), f32),
        pltpu.VMEM((3, depth, nx), f32),
        pltpu.VMEM((3, depth // 2, nx), f32),
        pltpu.VMEM((3, depth + 16, nx), f32),
        pltpu.VMEM((3, depth, nx), bf16),
        pltpu.VMEM((3 * depth, nx), bf16),
        pltpu.VMEM((6 * depth, nx), bf16),
        pltpu.VMEM((6 * depth, nx), bf16),
        pltpu.VMEM((max(depth, 6 * quarter), nx), bf16),
        pltpu.VMEM((6, quarter, nx), f32),
        pltpu.VMEM((6, depth, nx), bf16),
        pltpu.VMEM((6, depth, nx), f32),
        pltpu.VMEM((depth, nx), f32),
    ]
    scratch += [pltpu.VMEM((2, 8, nx), f32)] * 4
    scratch += [pltpu.VMEM((rows_v, nx), bf16)] * 4 + [pltpu.VMEM((rows_p, nx), bf16)] * 4
    scratch += [
        pltpu.VMEM((2, 8, nx), f32),
        pltpu.VMEM((2, 8, 128), f32),
        pltpu.VMEM((n - 1, 2, 8, 128), f32),
    ]
    scratch += [dma((3,)), dma((2, 2)), dma((2, 2)), dma((2, 4, 2)), dma((2, 4, 2)), dma((4,)), dma((4,))]
    scratch += [dma((3, n - 1))] * 2 + [dma((n - 1,))] * 2 + [dma((2,))] * 2 + [dma((n - 1,))] * 2
    nu_t, hat = pl.pallas_call(
        functools.partial(plane_kernel, n, ny, spans_v, spans_p),
        in_specs=[pl.BlockSpec(memory_space=pl.ANY)] + [vmem] * 6,
        out_specs=[vmem, vmem],
        out_shape=[
            jax.ShapeDtypeStruct((depth, nx), f32),
            jax.ShapeDtypeStruct((3, nz, width), bf16),
        ],
        scratch_shapes=scratch,
        compiler_params=pltpu.CompilerParams(
            collective_id=0, has_side_effects=True, vmem_limit_bytes=62 * 1024 * 1024
        ),
    )(velocity[:, 0], filter_table(nx), near, down_v, back_v, down_p, back_p)
    return nu_t[None], hat[:, None]


def solution(mesh):
    in_specs = (P(None, "py", "pz", None),)
    out_specs = (P("py", "pz", None), P(None, "py", None, "pz"))

    def step(velocity):
        depth, nx = velocity.shape[2:]
        banded = mesh.shape["pz"] == 4 and depth % 128 == 0 and nx % 512 == 0
        return plane_body(velocity) if banded else body(velocity)

    return jax.shard_map(step, mesh=mesh, in_specs=in_specs, out_specs=out_specs, check_vma=False)
```

```python
import functools
import math

import jax
import jax.numpy as jnp
import numpy as np
from jax import lax
from jax.experimental import pallas as pl
from jax.experimental.pallas import tpu as pltpu
from jax.sharding import PartitionSpec as P

index_pairs = ((0, 0), (1, 1), (2, 2), (0, 1), (0, 2), (1, 2))
pair_weights = (1.0, 1.0, 1.0, 2.0, 2.0, 2.0)
epsilon = 1e-06


def neighbours(first, last, axis, wrap):
    n = lax.axis_size(axis)
    up = [(i, (i + 1) % n) for i in range(n) if wrap or i + 1 < n]
    down = [(j, i) for i, j in up]
    return lax.ppermute(last, axis, up), lax.ppermute(first, axis, down)


def filter_taps(length):
    offsets = np.arange(length, dtype=np.int64)
    wavenumbers = np.arange(1, length // 4, dtype=np.int64)
    phase = offsets[:, None] * wavenumbers[None, :] % length
    kernel = (1.0 + 2.0 * np.cos(phase * (2.0 * math.pi / length)).sum(axis=1)) / length
    return kernel.astype(np.float32)


def filter_table(length):
    offsets = np.arange(length, dtype=np.int64)
    lagged = (offsets[:, None] - offsets[None, :]) % length
    return jnp.asarray(filter_taps(length)[lagged], dtype=jnp.float32).astype(jnp.bfloat16)


def strain(gradients):
    strain_parts = [0.5 * (gradients[b][a] + gradients[a][b]) for a, b in index_pairs]
    squares_sum = pair_weights[0] * strain_parts[0] * strain_parts[0]
    for weight, part_value in zip(pair_weights[1:], strain_parts[1:]):
        squares_sum = squares_sum + weight * part_value * part_value
    return strain_parts, jnp.sqrt(2.0 * squares_sum)


def filter_z_kernel(n, *refs):
    table, blocks, out = refs[0], refs[1 : 1 + n], refs[1 + n]
    width = blocks[0].shape[1]
    rows = min(512, out.shape[1])
    for top in range(0, out.shape[1], rows):
        total = None
        for s in range(n):
            term = jnp.dot(
                table[top : top + rows, s * width : (s + 1) * width],
                blocks[s][0],
                preferred_element_type=jnp.float32,
            )
            total = term if total is None else total + term
        out[0, top : top + rows, :] = total.astype(out.dtype)


def filter_z(table, blocks):
    n, (fields, width, columns) = len(blocks), blocks[0].shape
    length = table.shape[0]
    return pl.pallas_call(
        functools.partial(filter_z_kernel, n),
        grid=(fields,),
        in_specs=[pl.BlockSpec(table.shape, lambda f: (0, 0), pipeline_mode=pl.Buffered(1))]
        + [pl.BlockSpec((1, width, columns), lambda f: (f, 0, 0))] * n,
        out_specs=pl.BlockSpec((1, length, columns), lambda f: (f, 0, 0)),
        out_shape=jax.ShapeDtypeStruct((fields, length, columns), jnp.bfloat16),
        cost_estimate=pl.CostEstimate(
            flops=2 * fields * length * length * columns,
            bytes_accessed=4 * fields * length * columns + 2 * length * length,
            transcendentals=0,
        ),
    )(table, *blocks)


def coarse_kernel(hat, below, above, before, after, out, u):
    length, columns = hat.shape[1:]
    rows = min(64, length)
    for a in range(3):
        u[a, 8 : 8 + length, :] = hat[a].astype(jnp.float32)
        u[a, 0:8, :] = hat[a, length - 16 : length, :].astype(jnp.float32)[8:]
        u[a, 8 + length : 16 + length, :] = hat[a, 0:16, :].astype(jnp.float32)[:8]
    lane = lax.broadcasted_iota(jnp.int32, (rows, columns), 1)

    def tile(i, carry):
        top = pl.multiple_of(i * rows, rows)
        here = pl.ds(top, rows)
        grad = []
        for a in range(3):
            around = u[a, pl.ds(top, rows + 16), :]
            centre = around[8 : 8 + rows]
            left, right = pltpu.roll(centre, 1, 1), pltpu.roll(centre, columns - 1, 1)
            left = jnp.where(lane == 0, before[a, here, :].astype(jnp.float32), left)
            right = jnp.where(lane == columns - 1, after[a, here, :].astype(jnp.float32), right)
            slope_y = above[a, here, :].astype(jnp.float32) - below[a, here, :].astype(jnp.float32)
            slope_z = around[9 : 9 + rows] - around[7 : 7 + rows]
            grad.append([(right - left) * 0.5, slope_y * 0.5, slope_z * 0.5])
        parts, magnitude = strain(grad)
        for p, part in enumerate(parts):
            out[p, here, :] = 4.0 * magnitude * part
        return carry

    lax.fori_loop(0, length // rows, tile, 0)


def coarse_model(hat, below, above, before, after):
    _, length, columns = hat.shape
    vmem = pl.BlockSpec(memory_space=pltpu.VMEM)
    return pl.pallas_call(
        coarse_kernel,
        in_specs=[vmem] * 5,
        out_specs=vmem,
        out_shape=jax.ShapeDtypeStruct((6, length, columns), jnp.float32),
        scratch_shapes=[pltpu.VMEM((3, length + 16, columns), jnp.float32)],
        cost_estimate=pl.CostEstimate(
            flops=100 * length * columns, bytes_accessed=42 * length * columns, transcendentals=0
        ),
    )(hat, below, above, before, after)


def lilly_kernel(n, weight, *refs):
    table, blocks = refs[0], refs[1 : 1 + n]
    product, left, right, coarse, start, out = refs[1 + n :]
    width, columns = blocks[0].shape[1:]
    rows = min(256, product.shape[1])

    @pl.when(pl.program_id(0) == 0)
    def _():
        out[...] = start[...]

    for top in range(0, product.shape[1], rows):
        here = slice(top, top + rows)
        total = None
        for s in range(n):
            term = jnp.dot(
                table[here, s * width : (s + 1) * width],
                blocks[s][0],
                preferred_element_type=jnp.float32,
            )
            total = term if total is None else total + term
        fine = total.astype(jnp.bfloat16).astype(jnp.float32)
        model = fine - coarse[0, here, :]
        leonard = product[0, here, :].astype(jnp.float32) - left[0, here, :].astype(
            jnp.float32
        ) * right[0, here, :].astype(jnp.float32)
        for i, value in enumerate((leonard * model, model * model)):
            out[i] += weight * jnp.sum(value.reshape(rows // 8, 8, columns), axis=0)


def lilly(table, blocks, products, hat, coarse, first, start):
    n, (fields, width, columns) = len(blocks), blocks[0].shape
    length = table.shape[0]
    a0, b0 = index_pairs[first]
    a1, b1 = index_pairs[first + 1] if fields > 1 else (a0, b0)

    def plane(offset, step=1):
        return pl.BlockSpec((1, length, columns), lambda f: (offset + f * step, 0, 0))

    for f in range(fields):
        assert index_pairs[first + f] == (a0 + f * (a1 - a0), b0 + f * (b1 - b0))
        assert pair_weights[first + f] == pair_weights[first]
    sums = pl.BlockSpec(start.shape, lambda f: (0, 0, 0))
    return pl.pallas_call(
        functools.partial(lilly_kernel, n, pair_weights[first]),
        grid=(fields,),
        in_specs=[pl.BlockSpec(table.shape, lambda f: (0, 0), pipeline_mode=pl.Buffered(1))]
        + [pl.BlockSpec((1, width, columns), lambda f: (f, 0, 0))] * n
        + [plane(first), plane(a0, a1 - a0), plane(b0, b1 - b0), plane(first), sums],
        out_specs=sums,
        out_shape=jax.ShapeDtypeStruct(start.shape, jnp.float32),
        cost_estimate=pl.CostEstimate(
            flops=2 * fields * length * length * columns,
            bytes_accessed=12 * fields * length * columns + 2 * length * length,
            transcendentals=0,
        ),
    )(table, *blocks, products, hat, hat, coarse, start)


def coefficient_kernel(n, cells, part, out, held, send_sem, recv_sem):
    me = lax.axis_index("pz")
    barrier = pltpu.get_barrier_semaphore()
    others = [lax.rem(me + s, n) for s in range(1, n)]
    for other in others:
        pl.semaphore_signal(
            barrier, inc=1, device_id={"pz": other}, device_id_type=pl.DeviceIdType.MESH
        )
    pl.semaphore_wait(barrier, n - 1)
    copies = [
        pltpu.make_async_remote_copy(
            src_ref=part,
            dst_ref=held.at[s],
            send_sem=send_sem.at[s],
            recv_sem=recv_sem.at[s],
            device_id={"pz": other},
            device_id_type=pl.DeviceIdType.MESH,
        )
        for s, other in enumerate(others)
    ]
    for copy in copies:
        copy.start()
    total = part[...]
    for s, copy in enumerate(copies):
        copy.wait()
        total = total + held[s]
    mean = jnp.sum(jnp.sum(total, axis=2, keepdims=True), axis=1, keepdims=True) / cells
    value = mean[0] / (2.0 * (mean[1] + epsilon))
    out[...] = jnp.broadcast_to(value, out.shape)


def coefficient_of(part, cells, columns):
    n = lax.axis_size("pz")
    return pl.pallas_call(
        functools.partial(coefficient_kernel, n, cells),
        in_specs=[pl.BlockSpec(memory_space=pltpu.VMEM)],
        out_specs=pl.BlockSpec(memory_space=pltpu.VMEM),
        out_shape=jax.ShapeDtypeStruct((8, columns), jnp.float32),
        scratch_shapes=[
            pltpu.VMEM((n - 1,) + part.shape, jnp.float32),
            pltpu.SemaphoreType.DMA((n - 1,)),
            pltpu.SemaphoreType.DMA((n - 1,)),
        ],
        compiler_params=pltpu.CompilerParams(collective_id=0, has_side_effects=True),
    )(part)


def body(velocity):
    n, me = lax.axis_size("pz"), lax.axis_index("pz")
    v = velocity[:, 0]
    depth, nx = v.shape[1:]
    nz, width = depth * n, nx // n
    table_x = filter_table(nx)
    table_z = table_x if nz == nx else filter_table(nz)
    to_x = [
        lax.dynamic_slice_in_dim(table_x, lax.rem(me + s, n) * width, width, 1) for s in range(n)
    ]
    from_z = jnp.concatenate(
        [
            lax.dynamic_slice_in_dim(table_z, lax.rem(me - s + n, n) * depth, depth, 1)
            for s in range(n)
        ],
        axis=1,
    )
    order = list(range(n - 1, 0, -1))
    order.sort(key=lambda s: -min(s, n - s))

    def exchange(pieces):
        fields = jnp.stack([p.astype(jnp.bfloat16) for p in pieces])
        blocks = [None] * n
        for s in order + [0]:
            along = jnp.einsum(
                "fzx,xv->fzv", fields, to_x[s], preferred_element_type=jnp.float32
            ).astype(jnp.bfloat16)
            if s:
                along = lax.ppermute(along, "pz", [(i, (i + s) % n) for i in range(n)])
            blocks[s] = along
        return blocks

    blocks_v = exchange([v[a] for a in range(3)])
    below, above = neighbours(v, v, "py", False)
    before, after = neighbours(v[:, :1], v[:, -1:], "pz", True)
    blocks_p = exchange([v[a] * v[b] for a, b in index_pairs])

    padded = jnp.concatenate([before, v, after], axis=1)
    slope_x = (jnp.roll(v, -1, 2) - jnp.roll(v, 1, 2)) * 0.5
    slope_y = (above - below) * 0.5
    slope_z = (padded[:, 2:] - padded[:, :-2]) * 0.5
    grad = [[slope_x[a], slope_y[a], slope_z[a]] for a in range(3)]
    parts, magnitude = strain([[g[b] for b in range(3)] for g in grad])
    groups = ((0, 3), (3, 5), (5, 6))
    blocks_s = [
        exchange([magnitude * part for part in parts[first:last]]) for first, last in groups
    ]
    from_z, *local = lax.optimization_barrier((from_z, *[blocks[0] for blocks in blocks_s]))
    for blocks, own in zip(blocks_s, local):
        blocks[0] = own

    hat = filter_z(from_z, blocks_v)
    below, above = neighbours(hat, hat, "py", False)
    before, after = neighbours(hat[:, :, :1], hat[:, :, -1:], "pz", True)
    coarse = coarse_model(hat, below, above, before, after)
    products = filter_z(from_z, blocks_p)
    sums = jnp.zeros((2, 8, width), jnp.float32)
    for (first, _), blocks in zip(groups, blocks_s):
        sums = lilly(from_z, blocks, products, hat, coarse, first, sums)
    coefficient = coefficient_of(sums, nx * nz, nx)
    nu_t = magnitude.reshape(depth // 8, 8, nx) * coefficient
    return nu_t.reshape(1, depth, nx), hat[:, None]


MESH = pl.DeviceIdType.MESH


def round_up(value, step):
    return -(-value // step) * step


def cross_factors(length, width, offset):
    taps = filter_taps(length).astype(jnp.bfloat16).astype(np.float64)
    cells = np.arange(width)
    block = taps[(offset * width + cells[:, None] - cells[None, :]) % length]
    _, values, rows = np.linalg.svd(block)
    basis = rows[: int((values > 1e-3).sum())]
    probe = np.cos(0.37 * cells) + cells / width
    basis = basis * np.where(basis @ probe < 0, -1.0, 1.0)[:, None]
    basis = basis.astype(jnp.bfloat16).astype(np.float64)
    return np.linalg.lstsq(basis.T, block.T, rcond=None)[0].T, basis


def cross_tables(factors, fields, width):
    spans, top = {}, 0
    for s, (a, b) in factors.items():
        spans[s] = (top, round_up(fields * b.shape[0], 16))
        top += spans[s][1]
    down = np.zeros((top, fields * width))
    back = np.zeros((fields, width, top))
    for s, (a, b) in factors.items():
        rank = b.shape[0]
        for f in range(fields):
            rows = slice(spans[s][0] + f * rank, spans[s][0] + (f + 1) * rank)
            down[rows, f * width : (f + 1) * width] = b
            back[f][:, rows] = a
    return (
        jnp.asarray(down.astype(np.float32), dtype=jnp.bfloat16),
        jnp.asarray(back.astype(np.float32), dtype=jnp.bfloat16),
        spans,
    )


def plane_kernel(n, ny, chunks, spans, *refs):
    velocity, tables, (nu, hat) = refs[0], refs[1:5], refs[5:7]
    table, near, down, back = refs[7:11]
    v, below, above, detoured, u, hat_z = refs[11:17]
    along_v, along, along_y, x, scaled, leonard, coarse, fine = refs[17:25]
    edge_out, edge_in, hat_edge_out, hat_edge_in = refs[25:29]
    sent, held, held_below, held_above = refs[29:33]
    sums, sums_out, sums_in = refs[33:36]
    load_sem, edge_send, edge_recv, halo_send, halo_recv, detour_recv, onward_send = refs[36:43]
    cross_send, cross_recv, hat_send, hat_recv, pass_send, pass_recv, sum_send, sum_recv = refs[43:]

    iy, iz = lax.axis_index("py"), lax.axis_index("pz")
    depth, nx = nu.shape
    width = nx // n
    quarter = depth // chunks
    half = quarter // 2
    middle = ny // 2
    detours = ny == 8
    tile = 256
    columns = [slice(left, left + tile) for left in range(0, nx, tile)]
    f32, bf16 = jnp.float32, jnp.bfloat16

    def remote(src, dst, send, recv, **device):
        return pltpu.make_async_remote_copy(
            src_ref=src,
            dst_ref=dst,
            send_sem=send,
            recv_sem=recv,
            device_id=device,
            device_id_type=MESH,
        )

    def dot(a, b):
        return jnp.dot(a, b, preferred_element_type=f32)

    def ring(s):
        return lax.rem(iz + s, n)

    loads = [
        pltpu.make_async_copy(velocity.at[a], v.at[a, 8 : 8 + depth], load_sem.at[a])
        for a in range(3)
    ]
    for load in loads:
        load.start()
    fetches = [
        pltpu.make_async_copy(src, dst, load_sem.at[3 + i])
        for i, (src, dst) in enumerate(zip(tables, (table, near, down, back)))
    ]
    for fetch in fetches:
        fetch.start()
    barrier = pltpu.get_barrier_semaphore()
    for s in range(1, n):
        pl.semaphore_signal(barrier, inc=1, device_id={"pz": ring(s)}, device_id_type=MESH)
    for s in range(1, ny):
        pl.semaphore_signal(
            barrier, inc=1, device_id={"py": lax.rem(iy + s, ny)}, device_id_type=MESH
        )
    pl.semaphore_wait(barrier, n - 1 + ny - 1)
    for load in loads:
        load.wait()

    def halo(way, c, h):
        row = c * quarter + h * half
        return remote(
            v.at[:, pl.ds(pl.multiple_of(8 + row, 8), half)],
            (below, above)[way].at[:, pl.ds(pl.multiple_of(row, 8), half)],
            halo_send.at[way, c, h],
            halo_recv.at[way, c, h],
            py=iy + (1, -1)[way],
        )

    def detour(way, c):
        return remote(
            v.at[:, pl.ds(8 + c * quarter + half, half)],
            detoured.at[:, pl.ds(c * half, half)],
            halo_send.at[way, c, 1],
            detour_recv.at[c],
            py=iy + (middle, -middle)[way],
        )

    def onward(way, c):
        return remote(
            detoured.at[:, pl.ds(c * half, half)],
            (below, above)[way].at[:, pl.ds(c * quarter + half, half)],
            onward_send.at[c],
            halo_recv.at[way, c, 1],
            py=iy + (1 - middle, middle - 1)[way],
        )

    has_next = (iy < ny - 1, iy > 0)
    has_last = (iy > 0, iy < ny - 1)
    bridge = (iy == middle - 1, iy == middle)
    relay = (iy == ny - 1, iy == 0)

    for way in range(2):

        @pl.when(has_next[way])
        def _(way=way):
            for c in range(chunks):
                halo(way, c, 0).start()
                if detours:

                    @pl.when(bridge[way])
                    def _(way=way, c=c):
                        detour(way, c).start()

                    @pl.when(jnp.logical_not(bridge[way]))
                    def _(way=way, c=c):
                        halo(way, c, 1).start()

                else:
                    halo(way, c, 1).start()

    def pass_on(c):
        if detours:
            for way in range(2):

                @pl.when(relay[way])
                def _(way=way):
                    detour(way, c).wait_recv()
                    onward(way, c).start()

    def edges(source, out, into, which):
        for a in range(3):
            out[0, a : a + 1, :] = source[a, 7 + depth : 8 + depth, :]
            out[1, a : a + 1, :] = source[a, 8:9, :]
        return [
            remote(
                out.at[side],
                into.at[side],
                edge_send.at[which, side],
                edge_recv.at[which, side],
                pz=ring((1, n - 1)[side]),
            )
            for side in range(2)
        ]

    def fill_edges(into, target):
        for a in range(3):
            target[a, 7:8, :] = into[0, a : a + 1, :]
            target[a, 8 + depth : 9 + depth, :] = into[1, a : a + 1, :]

    rims = edges(v, edge_out, edge_in, 0)
    for rim in rims:
        rim.start()

    for empty, (rows, kept) in enumerate(((below, held_below), (above, held_above))):

        @pl.when(jnp.logical_not(has_last[empty]))
        def _(rows=rows, kept=kept):
            kept[...] = jnp.zeros_like(kept)

            def clear(i, carry):
                rows[:, pl.ds(pl.multiple_of(i * 8, 8), 8)] = jnp.zeros((3, 8, nx), f32)
                return carry

            lax.fori_loop(0, depth // 8, clear, 0)

    def along_x(dst, f, a, b):
        def convert(i, carry):
            row = pl.multiple_of(i * 32, 32)
            value = v[a, pl.ds(8 + row, 32)]
            if b is not None:
                value = value * v[b, pl.ds(8 + row, 32)]
            x[pl.ds(row, 32)] = value.astype(bf16)
            return carry

        lax.fori_loop(0, depth // 32, convert, 0)
        top = pl.multiple_of(f * depth, depth)
        for cols in columns:
            dst[pl.ds(top, depth), cols] = dot(x[0:depth], table[:, cols]).astype(bf16)

    def loop(count, step):
        lax.fori_loop(0, count, lambda i, carry: (step(i), carry)[1], 0)

    def cross(source, part, group):
        rows = slice(part * 3 * depth, (part + 1) * 3 * depth)
        for cols in columns:
            sent[group, :, cols] = dot(down[...], source[rows, cols]).astype(bf16)
        copies = [
            remote(
                sent.at[group, top : top + count],
                held.at[group, top : top + count],
                cross_send.at[group, s - 1],
                cross_recv.at[group, s - 1],
                pz=ring(s),
            )
            for s, (top, count) in spans.items()
        ]
        for copy in copies:
            copy.start()
        return copies

    def own_range(source, f, cols):
        top = pl.multiple_of(f * depth, depth)
        return dot(near[...], source[pl.ds(top, depth), cols])

    for fetch in fetches:
        fetch.wait()
    loop(3, lambda a: along_x(along_v, a, a, None))
    out_v = cross(along_v, 0, 0)
    pass_on(0)
    pass_on(1)
    loop(3, lambda i: along_x(along, i, i, i))
    out_p = cross(along, 0, 1)
    pass_on(2)
    pass_on(3)
    loop(2, lambda i: along_x(along, i + 3, 0, i + 1))
    along_x(along, 5, 1, 2)
    out_p += cross(along, 1, 2)
    pass_on(4)
    pass_on(5)

    for copy in out_v:
        copy.wait_recv()
    passes = [
        remote(held.at[0], (held_below, held_above)[way], pass_send.at[way], pass_recv.at[way],
               py=iy + (1, -1)[way])
        for way in range(2)
    ]
    for way in range(2):

        @pl.when(has_next[way])
        def _(way=way):
            passes[way].start()

    def smooth_velocity(a):
        for cols in columns:
            value = own_range(along_v, a, cols) + dot(back[a], held[0, :, cols])
            value = value.astype(bf16)
            hat_z[a, :, cols] = value
            u[a, 8 : 8 + depth, cols] = value.astype(f32)

    loop(3, smooth_velocity)
    pass_on(6)
    hat_rims = edges(u, hat_edge_out, hat_edge_in, 1)
    for rim in hat_rims:
        rim.start()

    def range_of(index):
        return pl.ds(pl.multiple_of(index * width, 128), width)

    mine = pl.ds(pl.multiple_of(iz * depth, depth), depth)
    turns = [
        remote(
            hat_z.at[:, :, range_of(ring(s))],
            hat.at[:, mine],
            hat_send.at[s - 1],
            hat_recv.at[s - 1],
            pz=ring(s),
        )
        for s in (2, 1, 3)
    ]
    for turn in turns:
        turn.start()
    for a in range(3):
        hat[a, mine, :] = hat_z[a, :, range_of(iz)]
    pass_on(7)

    for copy in out_p:
        copy.wait_recv()
    for p, (a, b) in enumerate(index_pairs):
        for cols in columns:
            value = own_range(along, p, cols) + dot(back[p % 3], held[1 + p // 3, :, cols])
            here = slice(8, 8 + depth)
            leonard[p, :, cols] = value.astype(bf16).astype(f32) - u[a, here, cols] * u[b, here, cols]

    for rim in rims:
        rim.wait_recv()
    fill_edges(edge_in, v)

    def strain_rows(source, lower, upper, row):
        grad = []
        here = pl.ds(row, 8)
        for a in range(3):
            around = source[a, pl.ds(row, 24)]
            centre = around[8:16]
            slope_x = pltpu.roll(centre, nx - 1, 1) - pltpu.roll(centre, 1, 1)
            slope_y = upper[a, here] - lower[a, here]
            slope_z = around[9:17] - around[7:15]
            grad.append([slope_x * 0.5, slope_y * 0.5, slope_z * 0.5])
        return strain(grad)

    def chunk(c):
        for way in range(2):

            @pl.when(has_last[way])
            def _(way=way):
                halo(way, c, 0).wait_recv()
                halo(way, c, 1).wait_recv()

        base = pl.multiple_of(c * quarter, quarter)

        def strain_tile(i):
            row = pl.multiple_of(base + i * 8, 8)
            parts, magnitude = strain_rows(v, below, above, row)
            nu[pl.ds(row, 8)] = magnitude
            for p in range(6):
                scaled[p, pl.ds(pl.multiple_of(i * 8, 8), 8)] = magnitude * parts[p]

        loop(quarter // 8, strain_tile)

        def project(pick, dst):
            def convert(p):
                x[pl.ds(pl.multiple_of(p * quarter, quarter), quarter)] = pick(p).astype(bf16)

            if isinstance(pick, list):
                for p, rows in enumerate(pick):
                    top = p * quarter
                    x[top : top + quarter] = rows[0][rows[1], pl.ds(base, quarter)].astype(bf16)
            else:
                loop(6, convert)
            for cols in columns:
                value = dot(x[0 : 6 * quarter], table[:, cols]).astype(bf16)
                for p in range(6):
                    dst[pl.ds(pl.multiple_of(p * depth + base, quarter), quarter), cols] = value[
                        p * quarter : (p + 1) * quarter
                    ]

        project(lambda p: scaled[p], along)
        project([(rows, a) for rows in (below, above) for a in range(3)], along_y)

    loop(chunks, chunk)
    out_s = [cross(along, 0, 3), cross(along, 1, 4)]

    def near_part(p):
        for cols in columns:
            fine[p, :, cols] = own_range(along, p, cols)

    loop(6, near_part)

    for way, (rows, kept) in enumerate(((below, held_below), (above, held_above))):

        @pl.when(has_last[way])
        def _(way=way):
            passes[way].wait_recv()

        def smooth_rows(a, way=way, rows=rows, kept=kept):
            for cols in columns:
                value = (
                    dot(near[...], along_y[pl.ds(pl.multiple_of((way * 3 + a) * depth, depth), depth), cols])
                    + dot(back[a], kept[:, cols])
                )
                rows[a, :, cols] = value.astype(bf16).astype(f32)

        loop(3, smooth_rows)

    for rim in hat_rims:
        rim.wait_recv()
    fill_edges(hat_edge_in, u)

    def coarse_tile(i):
        row = pl.multiple_of(i * 8, 8)
        parts, magnitude = strain_rows(u, below, above, row)
        for p in range(6):
            coarse[p, pl.ds(row, 8)] = 4.0 * magnitude * parts[p]

    loop(depth // 8, coarse_tile)

    sums[...] = jnp.zeros_like(sums)
    for p in range(6):
        if p % 3 == 0:
            for copy in out_s[p // 3]:
                copy.wait_recv()
        for cols in columns:
            value = fine[p, :, cols] + dot(back[p % 3], held[3 + p // 3, :, cols])
            model = value.astype(bf16).astype(f32) - coarse[p, :, cols]
            for i, value in enumerate((leonard[p, :, cols] * model, model * model)):
                value = jnp.sum(value.reshape(depth // 8, 8, tile), axis=0)
                sums[i, :, cols] += pair_weights[p] * value

    for i in range(2):
        value = sums[i]
        part = value[:, 0:128]
        for left in range(128, nx, 128):
            part = part + value[:, left : left + 128]
        sums_out[i] = part
    shares = [
        remote(sums_out, sums_in.at[s - 1], sum_send.at[s - 1], sum_recv.at[s - 1], pz=ring(s))
        for s in range(1, n)
    ]
    for share in shares:
        share.start()
    total = sums_out[...]
    for s, share in enumerate(shares):
        share.wait_recv()
        total = total + sums_in[s]
    cells = float(nx * depth * n)
    mean = jnp.sum(jnp.sum(total, axis=2, keepdims=True), axis=1, keepdims=True) / cells
    coefficient = jnp.broadcast_to(mean[0] / (2.0 * (mean[1] + epsilon)), (8, nx))

    def scale(i):
        here = pl.ds(pl.multiple_of(i * 8, 8), 8)
        nu[here] = nu[here] * coefficient

    loop(depth // 8, scale)

    for turn in turns:
        turn.wait_recv()
    for copy in rims + hat_rims + out_v + out_p + out_s[0] + out_s[1] + turns + shares:
        copy.wait_send()
    for way in range(2):

        @pl.when(has_next[way])
        def _(way=way):
            passes[way].wait_send()
            for c in range(chunks):
                halo(way, c, 0).wait_send()
                halo(way, c, 1).wait_send()

        if detours:

            @pl.when(relay[way])
            def _(way=way):
                for c in range(chunks):
                    onward(way, c).wait_send()


def plane_body(velocity):
    n, ny = lax.axis_size("pz"), lax.axis_size("py")
    depth, nx = velocity.shape[2:]
    nz, width = depth * n, nx // n
    chunks = 8
    quarter = depth // chunks
    down, back, spans = cross_tables(
        {s: cross_factors(nz, depth, s) for s in (1, n - 1, 2)}, 3, depth
    )
    cells = np.arange(depth)
    near = filter_taps(nz)[(cells[:, None] - cells[None, :]) % nz]
    near = jnp.asarray(near, dtype=jnp.float32).astype(jnp.bfloat16)
    tables = (filter_table(nx), near, down, back)
    f32, bf16 = jnp.float32, jnp.bfloat16
    vmem, anywhere = pl.BlockSpec(memory_space=pltpu.VMEM), pl.BlockSpec(memory_space=pl.ANY)
    dma = pltpu.SemaphoreType.DMA
    rows = down.shape[0]
    scratch = [pltpu.VMEM(t.shape, bf16) for t in tables]
    scratch += [
        pltpu.VMEM((3, depth + 16, nx), f32),
        pltpu.VMEM((3, depth, nx), f32),
        pltpu.VMEM((3, depth, nx), f32),
        pltpu.VMEM((3, depth // 2, nx), f32),
        pltpu.VMEM((3, depth + 16, nx), f32),
        pltpu.VMEM((3, depth, nx), bf16),
        pltpu.VMEM((3 * depth, nx), bf16),
        pltpu.VMEM((6 * depth, nx), bf16),
        pltpu.VMEM((6 * depth, nx), bf16),
        pltpu.VMEM((max(depth, 6 * quarter), nx), bf16),
        pltpu.VMEM((6, quarter, nx), f32),
        pltpu.VMEM((6, depth, nx), f32),
        pltpu.VMEM((6, depth, nx), f32),
        pltpu.VMEM((6, depth, nx), f32),
    ]
    scratch += [pltpu.VMEM((2, 8, nx), f32)] * 4
    scratch += [pltpu.VMEM((5, rows, nx), bf16)] * 2 + [pltpu.VMEM((rows, nx), bf16)] * 2
    scratch += [
        pltpu.VMEM((2, 8, nx), f32),
        pltpu.VMEM((2, 8, 128), f32),
        pltpu.VMEM((n - 1, 2, 8, 128), f32),
    ]
    scratch += [dma((7,)), dma((2, 2)), dma((2, 2)), dma((2, chunks, 2)), dma((2, chunks, 2))]
    scratch += [dma((chunks,)), dma((chunks,)), dma((5, n - 1)), dma((5, n - 1))]
    scratch += [dma((n - 1,))] * 2 + [dma((2,))] * 2 + [dma((n - 1,))] * 2
    nu_t, hat = pl.pallas_call(
        functools.partial(plane_kernel, n, ny, chunks, spans),
        in_specs=[anywhere] * 5,
        out_specs=[vmem, vmem],
        out_shape=[
            jax.ShapeDtypeStruct((depth, nx), f32),
            jax.ShapeDtypeStruct((3, nz, width), bf16),
        ],
        scratch_shapes=scratch,
        compiler_params=pltpu.CompilerParams(
            collective_id=0, has_side_effects=True, vmem_limit_bytes=54 * 1024 * 1024
        ),
    )(velocity[:, 0], *tables)
    return nu_t[None], hat[:, None]


def solution(mesh):
    in_specs = (P(None, "py", "pz", None),)
    out_specs = (P("py", "pz", None), P(None, "py", None, "pz"))

    def step(velocity):
        depth, nx = velocity.shape[2:]
        banded = mesh.shape["pz"] == 4 and depth % 128 == 0 and nx % 512 == 0
        return plane_body(velocity) if banded else body(velocity)

    return jax.shard_map(step, mesh=mesh, in_specs=in_specs, out_specs=out_specs, check_vma=False)
```

```python
import functools
import math

import jax
import jax.numpy as jnp
import numpy as np
from jax import lax
from jax.experimental import pallas as pl
from jax.experimental.pallas import tpu as pltpu
from jax.sharding import PartitionSpec as P

index_pairs = ((0, 0), (1, 1), (2, 2), (0, 1), (0, 2), (1, 2))
pair_weights = (1.0, 1.0, 1.0, 2.0, 2.0, 2.0)
epsilon = 1e-06


def neighbours(first, last, axis, wrap):
    n = lax.axis_size(axis)
    up = [(i, (i + 1) % n) for i in range(n) if wrap or i + 1 < n]
    down = [(j, i) for i, j in up]
    return lax.ppermute(last, axis, up), lax.ppermute(first, axis, down)


def filter_taps(length):
    offsets = np.arange(length, dtype=np.int64)
    wavenumbers = np.arange(1, length // 4, dtype=np.int64)
    phase = offsets[:, None] * wavenumbers[None, :] % length
    kernel = (1.0 + 2.0 * np.cos(phase * (2.0 * math.pi / length)).sum(axis=1)) / length
    return kernel.astype(np.float32)


def filter_table(length):
    offsets = np.arange(length, dtype=np.int64)
    lagged = (offsets[:, None] - offsets[None, :]) % length
    return jnp.asarray(filter_taps(length)[lagged], dtype=jnp.float32).astype(jnp.bfloat16)


def strain(gradients):
    strain_parts = [0.5 * (gradients[b][a] + gradients[a][b]) for a, b in index_pairs]
    squares_sum = pair_weights[0] * strain_parts[0] * strain_parts[0]
    for weight, part_value in zip(pair_weights[1:], strain_parts[1:]):
        squares_sum = squares_sum + weight * part_value * part_value
    return strain_parts, jnp.sqrt(2.0 * squares_sum)


def filter_z_kernel(n, *refs):
    table, blocks, out = refs[0], refs[1 : 1 + n], refs[1 + n]
    width = blocks[0].shape[1]
    rows = min(512, out.shape[1])
    for top in range(0, out.shape[1], rows):
        total = None
        for s in range(n):
            term = jnp.dot(
                table[top : top + rows, s * width : (s + 1) * width],
                blocks[s][0],
                preferred_element_type=jnp.float32,
            )
            total = term if total is None else total + term
        out[0, top : top + rows, :] = total.astype(out.dtype)


def filter_z(table, blocks):
    n, (fields, width, columns) = len(blocks), blocks[0].shape
    length = table.shape[0]
    return pl.pallas_call(
        functools.partial(filter_z_kernel, n),
        grid=(fields,),
        in_specs=[pl.BlockSpec(table.shape, lambda f: (0, 0), pipeline_mode=pl.Buffered(1))]
        + [pl.BlockSpec((1, width, columns), lambda f: (f, 0, 0))] * n,
        out_specs=pl.BlockSpec((1, length, columns), lambda f: (f, 0, 0)),
        out_shape=jax.ShapeDtypeStruct((fields, length, columns), jnp.bfloat16),
        cost_estimate=pl.CostEstimate(
            flops=2 * fields * length * length * columns,
            bytes_accessed=4 * fields * length * columns + 2 * length * length,
            transcendentals=0,
        ),
    )(table, *blocks)


def coarse_kernel(hat, below, above, before, after, out, u):
    length, columns = hat.shape[1:]
    rows = min(64, length)
    for a in range(3):
        u[a, 8 : 8 + length, :] = hat[a].astype(jnp.float32)
        u[a, 0:8, :] = hat[a, length - 16 : length, :].astype(jnp.float32)[8:]
        u[a, 8 + length : 16 + length, :] = hat[a, 0:16, :].astype(jnp.float32)[:8]
    lane = lax.broadcasted_iota(jnp.int32, (rows, columns), 1)

    def tile(i, carry):
        top = pl.multiple_of(i * rows, rows)
        here = pl.ds(top, rows)
        grad = []
        for a in range(3):
            around = u[a, pl.ds(top, rows + 16), :]
            centre = around[8 : 8 + rows]
            left, right = pltpu.roll(centre, 1, 1), pltpu.roll(centre, columns - 1, 1)
            left = jnp.where(lane == 0, before[a, here, :].astype(jnp.float32), left)
            right = jnp.where(lane == columns - 1, after[a, here, :].astype(jnp.float32), right)
            slope_y = above[a, here, :].astype(jnp.float32) - below[a, here, :].astype(jnp.float32)
            slope_z = around[9 : 9 + rows] - around[7 : 7 + rows]
            grad.append([(right - left) * 0.5, slope_y * 0.5, slope_z * 0.5])
        parts, magnitude = strain(grad)
        for p, part in enumerate(parts):
            out[p, here, :] = 4.0 * magnitude * part
        return carry

    lax.fori_loop(0, length // rows, tile, 0)


def coarse_model(hat, below, above, before, after):
    _, length, columns = hat.shape
    vmem = pl.BlockSpec(memory_space=pltpu.VMEM)
    return pl.pallas_call(
        coarse_kernel,
        in_specs=[vmem] * 5,
        out_specs=vmem,
        out_shape=jax.ShapeDtypeStruct((6, length, columns), jnp.float32),
        scratch_shapes=[pltpu.VMEM((3, length + 16, columns), jnp.float32)],
        cost_estimate=pl.CostEstimate(
            flops=100 * length * columns, bytes_accessed=42 * length * columns, transcendentals=0
        ),
    )(hat, below, above, before, after)


def lilly_kernel(n, weight, *refs):
    table, blocks = refs[0], refs[1 : 1 + n]
    product, left, right, coarse, start, out = refs[1 + n :]
    width, columns = blocks[0].shape[1:]
    rows = min(256, product.shape[1])

    @pl.when(pl.program_id(0) == 0)
    def _():
        out[...] = start[...]

    for top in range(0, product.shape[1], rows):
        here = slice(top, top + rows)
        total = None
        for s in range(n):
            term = jnp.dot(
                table[here, s * width : (s + 1) * width],
                blocks[s][0],
                preferred_element_type=jnp.float32,
            )
            total = term if total is None else total + term
        fine = total.astype(jnp.bfloat16).astype(jnp.float32)
        model = fine - coarse[0, here, :]
        leonard = product[0, here, :].astype(jnp.float32) - left[0, here, :].astype(
            jnp.float32
        ) * right[0, here, :].astype(jnp.float32)
        for i, value in enumerate((leonard * model, model * model)):
            out[i] += weight * jnp.sum(value.reshape(rows // 8, 8, columns), axis=0)


def lilly(table, blocks, products, hat, coarse, first, start):
    n, (fields, width, columns) = len(blocks), blocks[0].shape
    length = table.shape[0]
    a0, b0 = index_pairs[first]
    a1, b1 = index_pairs[first + 1] if fields > 1 else (a0, b0)

    def plane(offset, step=1):
        return pl.BlockSpec((1, length, columns), lambda f: (offset + f * step, 0, 0))

    for f in range(fields):
        assert index_pairs[first + f] == (a0 + f * (a1 - a0), b0 + f * (b1 - b0))
        assert pair_weights[first + f] == pair_weights[first]
    sums = pl.BlockSpec(start.shape, lambda f: (0, 0, 0))
    return pl.pallas_call(
        functools.partial(lilly_kernel, n, pair_weights[first]),
        grid=(fields,),
        in_specs=[pl.BlockSpec(table.shape, lambda f: (0, 0), pipeline_mode=pl.Buffered(1))]
        + [pl.BlockSpec((1, width, columns), lambda f: (f, 0, 0))] * n
        + [plane(first), plane(a0, a1 - a0), plane(b0, b1 - b0), plane(first), sums],
        out_specs=sums,
        out_shape=jax.ShapeDtypeStruct(start.shape, jnp.float32),
        cost_estimate=pl.CostEstimate(
            flops=2 * fields * length * length * columns,
            bytes_accessed=12 * fields * length * columns + 2 * length * length,
            transcendentals=0,
        ),
    )(table, *blocks, products, hat, hat, coarse, start)


def coefficient_kernel(n, cells, part, out, held, send_sem, recv_sem):
    me = lax.axis_index("pz")
    barrier = pltpu.get_barrier_semaphore()
    others = [lax.rem(me + s, n) for s in range(1, n)]
    for other in others:
        pl.semaphore_signal(
            barrier, inc=1, device_id={"pz": other}, device_id_type=pl.DeviceIdType.MESH
        )
    pl.semaphore_wait(barrier, n - 1)
    copies = [
        pltpu.make_async_remote_copy(
            src_ref=part,
            dst_ref=held.at[s],
            send_sem=send_sem.at[s],
            recv_sem=recv_sem.at[s],
            device_id={"pz": other},
            device_id_type=pl.DeviceIdType.MESH,
        )
        for s, other in enumerate(others)
    ]
    for copy in copies:
        copy.start()
    total = part[...]
    for s, copy in enumerate(copies):
        copy.wait()
        total = total + held[s]
    mean = jnp.sum(jnp.sum(total, axis=2, keepdims=True), axis=1, keepdims=True) / cells
    value = mean[0] / (2.0 * (mean[1] + epsilon))
    out[...] = jnp.broadcast_to(value, out.shape)


def coefficient_of(part, cells, columns):
    n = lax.axis_size("pz")
    return pl.pallas_call(
        functools.partial(coefficient_kernel, n, cells),
        in_specs=[pl.BlockSpec(memory_space=pltpu.VMEM)],
        out_specs=pl.BlockSpec(memory_space=pltpu.VMEM),
        out_shape=jax.ShapeDtypeStruct((8, columns), jnp.float32),
        scratch_shapes=[
            pltpu.VMEM((n - 1,) + part.shape, jnp.float32),
            pltpu.SemaphoreType.DMA((n - 1,)),
            pltpu.SemaphoreType.DMA((n - 1,)),
        ],
        compiler_params=pltpu.CompilerParams(collective_id=0, has_side_effects=True),
    )(part)


def body(velocity):
    n, me = lax.axis_size("pz"), lax.axis_index("pz")
    v = velocity[:, 0]
    depth, nx = v.shape[1:]
    nz, width = depth * n, nx // n
    table_x = filter_table(nx)
    table_z = table_x if nz == nx else filter_table(nz)
    to_x = [
        lax.dynamic_slice_in_dim(table_x, lax.rem(me + s, n) * width, width, 1) for s in range(n)
    ]
    from_z = jnp.concatenate(
        [
            lax.dynamic_slice_in_dim(table_z, lax.rem(me - s + n, n) * depth, depth, 1)
            for s in range(n)
        ],
        axis=1,
    )
    order = list(range(n - 1, 0, -1))
    order.sort(key=lambda s: -min(s, n - s))

    def exchange(pieces):
        fields = jnp.stack([p.astype(jnp.bfloat16) for p in pieces])
        blocks = [None] * n
        for s in order + [0]:
            along = jnp.einsum(
                "fzx,xv->fzv", fields, to_x[s], preferred_element_type=jnp.float32
            ).astype(jnp.bfloat16)
            if s:
                along = lax.ppermute(along, "pz", [(i, (i + s) % n) for i in range(n)])
            blocks[s] = along
        return blocks

    blocks_v = exchange([v[a] for a in range(3)])
    below, above = neighbours(v, v, "py", False)
    before, after = neighbours(v[:, :1], v[:, -1:], "pz", True)
    blocks_p = exchange([v[a] * v[b] for a, b in index_pairs])

    padded = jnp.concatenate([before, v, after], axis=1)
    slope_x = (jnp.roll(v, -1, 2) - jnp.roll(v, 1, 2)) * 0.5
    slope_y = (above - below) * 0.5
    slope_z = (padded[:, 2:] - padded[:, :-2]) * 0.5
    grad = [[slope_x[a], slope_y[a], slope_z[a]] for a in range(3)]
    parts, magnitude = strain([[g[b] for b in range(3)] for g in grad])
    groups = ((0, 3), (3, 5), (5, 6))
    blocks_s = [
        exchange([magnitude * part for part in parts[first:last]]) for first, last in groups
    ]
    from_z, *local = lax.optimization_barrier((from_z, *[blocks[0] for blocks in blocks_s]))
    for blocks, own in zip(blocks_s, local):
        blocks[0] = own

    hat = filter_z(from_z, blocks_v)
    below, above = neighbours(hat, hat, "py", False)
    before, after = neighbours(hat[:, :, :1], hat[:, :, -1:], "pz", True)
    coarse = coarse_model(hat, below, above, before, after)
    products = filter_z(from_z, blocks_p)
    sums = jnp.zeros((2, 8, width), jnp.float32)
    for (first, _), blocks in zip(groups, blocks_s):
        sums = lilly(from_z, blocks, products, hat, coarse, first, sums)
    coefficient = coefficient_of(sums, nx * nz, nx)
    nu_t = magnitude.reshape(depth // 8, 8, nx) * coefficient
    return nu_t.reshape(1, depth, nx), hat[:, None]


MESH = pl.DeviceIdType.MESH


def round_up(value, step):
    return -(-value // step) * step


def cross_factors(length, width, offset):
    taps = filter_taps(length).astype(jnp.bfloat16).astype(np.float64)
    cells = np.arange(width)
    block = taps[(offset * width + cells[:, None] - cells[None, :]) % length]
    _, values, rows = np.linalg.svd(block)
    basis = rows[: int((values > 1e-3).sum())]
    probe = np.cos(0.37 * cells) + cells / width
    basis = basis * np.where(basis @ probe < 0, -1.0, 1.0)[:, None]
    basis = basis.astype(jnp.bfloat16).astype(np.float64)
    return np.linalg.lstsq(basis.T, block.T, rcond=None)[0].T, basis


def cross_tables(factors, fields, width):
    spans, top = {}, 0
    for s, (a, b) in factors.items():
        spans[s] = (top, round_up(fields * b.shape[0], 16))
        top += spans[s][1]
    down = np.zeros((top, fields * width))
    back = np.zeros((fields, width, top))
    for s, (a, b) in factors.items():
        rank = b.shape[0]
        for f in range(fields):
            rows = slice(spans[s][0] + f * rank, spans[s][0] + (f + 1) * rank)
            down[rows, f * width : (f + 1) * width] = b
            back[f][:, rows] = a
    return (
        jnp.asarray(down.astype(np.float32), dtype=jnp.bfloat16),
        jnp.asarray(back.astype(np.float32), dtype=jnp.bfloat16),
        spans,
    )


def plane_kernel(n, ny, chunks, spans, *refs):
    velocity, tables, (nu, hat) = refs[0], refs[1:5], refs[5:7]
    table, near, down, back = refs[7:11]
    v, halo_out, halo_in, detoured, u, hat_z = refs[11:17]
    along_v, along, along_y, along_s, x, leonard, coarse, fine = refs[17:25]
    edge_out, edge_in, hat_edge_out, hat_edge_in = refs[25:29]
    sent, held, held_below, held_above = refs[29:33]
    sums, sums_out, sums_in = refs[33:36]
    load_sem, edge_send, edge_recv, halo_send, halo_recv, detour_recv, onward_send = refs[36:43]
    cross_send, cross_recv, hat_send, hat_recv, pass_send, pass_recv, sum_send, sum_recv = refs[43:]

    iy, iz = lax.axis_index("py"), lax.axis_index("pz")
    depth, nx = nu.shape
    width = nx // n
    quarter = depth // chunks
    half = quarter // 2
    middle = ny // 2
    detours = ny == 8
    tile = 256
    columns = [slice(left, left + tile) for left in range(0, nx, tile)]
    f32, bf16 = jnp.float32, jnp.bfloat16

    def remote(src, dst, send, recv, **device):
        return pltpu.make_async_remote_copy(
            src_ref=src,
            dst_ref=dst,
            send_sem=send,
            recv_sem=recv,
            device_id=device,
            device_id_type=MESH,
        )

    def dot(a, b):
        return jnp.dot(a, b, preferred_element_type=f32)

    def ring(s):
        return lax.rem(iz + s, n)

    loads = [
        pltpu.make_async_copy(velocity.at[a], v.at[a, 8 : 8 + depth], load_sem.at[a])
        for a in range(3)
    ]
    for load in loads:
        load.start()
    fetches = [
        pltpu.make_async_copy(src, dst, load_sem.at[3 + i])
        for i, (src, dst) in enumerate(zip(tables, (table, near, down, back)))
    ]
    for fetch in fetches:
        fetch.start()
    barrier = pltpu.get_barrier_semaphore()
    for s in range(1, n):
        pl.semaphore_signal(barrier, inc=1, device_id={"pz": ring(s)}, device_id_type=MESH)
    for s in range(1, ny):
        pl.semaphore_signal(
            barrier, inc=1, device_id={"py": lax.rem(iy + s, ny)}, device_id_type=MESH
        )

    def loop(count, step):
        lax.fori_loop(0, count, lambda i, carry: (step(i), carry)[1], 0)

    for a in range(3):
        loads[a].wait()

        def split(i, a=a):
            row = pl.multiple_of(i * 16, 16)
            value = v[a, pl.ds(8 + row, 16)]
            high = value.astype(bf16)
            halo_out[0, a, pl.ds(row, 16)] = high
            halo_out[1, a, pl.ds(row, 16)] = (value - high.astype(f32)).astype(bf16)

        loop(depth // 16, split)
    pl.semaphore_wait(barrier, n - 1 + ny - 1)

    def halo(way, part, c, h):
        rows = pl.ds(pl.multiple_of(c * quarter + h * half, half), half)
        return remote(
            halo_out.at[part, :, rows],
            halo_in.at[way, part, :, rows],
            halo_send.at[way, part, c, h],
            halo_recv.at[way, part, c, h],
            py=iy + (1, -1)[way],
        )

    def detour(way, part, c):
        return remote(
            halo_out.at[part, :, pl.ds(c * quarter + half, half)],
            detoured.at[part, :, pl.ds(c * half, half)],
            halo_send.at[way, part, c, 1],
            detour_recv.at[part, c],
            py=iy + (middle, -middle)[way],
        )

    def onward(way, part, c):
        return remote(
            detoured.at[part, :, pl.ds(c * half, half)],
            halo_in.at[way, part, :, pl.ds(c * quarter + half, half)],
            onward_send.at[part, c],
            halo_recv.at[way, part, c, 1],
            py=iy + (1 - middle, middle - 1)[way],
        )

    pieces = [(part, c) for part in range(2) for c in range(chunks)]
    has_next = (iy < ny - 1, iy > 0)
    has_last = (iy > 0, iy < ny - 1)
    bridge = (iy == middle - 1, iy == middle)
    relay = (iy == ny - 1, iy == 0)

    for way in range(2):

        @pl.when(has_next[way])
        def _(way=way):
            for part, c in pieces:
                halo(way, part, c, 0).start()
                if detours:

                    @pl.when(bridge[way])
                    def _(way=way, part=part, c=c):
                        detour(way, part, c).start()

                    @pl.when(jnp.logical_not(bridge[way]))
                    def _(way=way, part=part, c=c):
                        halo(way, part, c, 1).start()

                else:
                    halo(way, part, c, 1).start()

    def pass_on(first, last):
        if detours:
            for way in range(2):

                @pl.when(relay[way])
                def _(way=way):
                    for part, c in pieces[first:last]:
                        detour(way, part, c).wait_recv()
                        onward(way, part, c).start()

    def edges(source, out, into, which):
        for a in range(3):
            out[0, a : a + 1, :] = source[a, 7 + depth : 8 + depth, :]
            out[1, a : a + 1, :] = source[a, 8:9, :]
        return [
            remote(
                out.at[side],
                into.at[side],
                edge_send.at[which, side],
                edge_recv.at[which, side],
                pz=ring((1, n - 1)[side]),
            )
            for side in range(2)
        ]

    def fill_edges(into, target):
        for a in range(3):
            target[a, 7:8, :] = into[0, a : a + 1, :]
            target[a, 8 + depth : 9 + depth, :] = into[1, a : a + 1, :]

    rims = edges(v, edge_out, edge_in, 0)
    for rim in rims:
        rim.start()

    for way, kept in enumerate((held_below, held_above)):

        @pl.when(jnp.logical_not(has_last[way]))
        def _(way=way, kept=kept):
            kept[...] = jnp.zeros_like(kept)

            def clear(i):
                rows = pl.ds(pl.multiple_of(i * 16, 16), 16)
                halo_in[way, :, :, rows] = jnp.zeros((2, 3, 16, nx), bf16)

            loop(depth // 16, clear)

    def along_x(dst, f, rows):
        top = pl.multiple_of(f * depth, depth)
        for cols in columns:
            dst[pl.ds(top, depth), cols] = dot(rows[...], table[:, cols]).astype(bf16)

    def along_product(f, a, b):
        def convert(i):
            row = pl.multiple_of(i * 32, 32)
            here = pl.ds(8 + row, 32)
            x[pl.ds(row, 32)] = (v[a, here] * v[b, here]).astype(bf16)

        loop(depth // 32, convert)
        along_x(along, f, x.at[0:depth])

    def cross(source, part, group):
        rows = slice(part * 3 * depth, (part + 1) * 3 * depth)
        for cols in columns:
            sent[group, :, cols] = dot(down[...], source[rows, cols]).astype(bf16)
        copies = [
            remote(
                sent.at[group, top : top + count],
                held.at[group, top : top + count],
                cross_send.at[group, s - 1],
                cross_recv.at[group, s - 1],
                pz=ring(s),
            )
            for s, (top, count) in spans.items()
        ]
        for copy in copies:
            copy.start()
        return copies

    def own_range(source, f, cols):
        top = pl.multiple_of(f * depth, depth)
        return dot(near[...], source[pl.ds(top, depth), cols])

    for fetch in fetches:
        fetch.wait()
    loop(3, lambda a: along_x(along_v, a, halo_out.at[0, a]))
    out_v = cross(along_v, 0, 0)
    pass_on(0, chunks // 2)
    loop(3, lambda i: along_product(i, i, i))
    out_p = cross(along, 0, 1)
    pass_on(chunks // 2, chunks)
    loop(2, lambda i: along_product(i + 3, 0, i + 1))
    along_product(5, 1, 2)
    out_p += cross(along, 1, 2)
    pass_on(chunks, chunks + 2)

    for copy in out_v:
        copy.wait_recv()
    passes = [
        remote(held.at[0], (held_below, held_above)[way], pass_send.at[way], pass_recv.at[way],
               py=iy + (1, -1)[way])
        for way in range(2)
    ]
    for way in range(2):

        @pl.when(has_next[way])
        def _(way=way):
            passes[way].start()

    def smooth_velocity(a):
        for cols in columns:
            value = own_range(along_v, a, cols) + dot(back[a], held[0, :, cols])
            value = value.astype(bf16)
            hat_z[a, :, cols] = value
            u[a, 8 : 8 + depth, cols] = value.astype(f32)

    loop(3, smooth_velocity)
    pass_on(chunks + 2, chunks + chunks // 2)
    hat_rims = edges(u, hat_edge_out, hat_edge_in, 1)
    for rim in hat_rims:
        rim.start()

    def range_of(index):
        return pl.ds(pl.multiple_of(index * width, 128), width)

    mine = pl.ds(pl.multiple_of(iz * depth, depth), depth)
    turns = [
        remote(
            hat_z.at[:, :, range_of(ring(s))],
            hat.at[:, mine],
            hat_send.at[s - 1],
            hat_recv.at[s - 1],
            pz=ring(s),
        )
        for s in (2, 1, 3)
    ]
    for turn in turns:
        turn.start()
    for a in range(3):
        hat[a, mine, :] = hat_z[a, :, range_of(iz)]
    pass_on(chunks + chunks // 2, 2 * chunks)

    def arrived(part, c):
        for way in range(2):

            @pl.when(has_last[way])
            def _(way=way):
                halo(way, part, c, 0).wait_recv()
                halo(way, part, c, 1).wait_recv()

    def strain_rows(source, slopes_y, row):
        grad = []
        for a in range(3):
            around = source[a, pl.ds(row, 24)]
            centre = around[8:16]
            slope_x = pltpu.roll(centre, nx - 1, 1) - pltpu.roll(centre, 1, 1)
            grad.append([slope_x, slopes_y[a], around[9:17] - around[7:15]])
        twice = [grad[a][b] if a == b else grad[a][b] + grad[b][a] for a, b in index_pairs]
        total = None
        for value, (a, b) in zip(twice, index_pairs):
            term = value * value * (2.0 if a == b else 1.0)
            total = term if total is None else total + term
        parts = [value * (0.5 if a == b else 0.25) for value, (a, b) in zip(twice, index_pairs)]
        return jnp.sqrt(total), parts

    loop(chunks, lambda c: arrived(0, c))
    for way in range(2):
        loop(3, lambda a, way=way: along_x(along_y, way * 3 + a, halo_in.at[way, 0, a]))
    for way, kept in enumerate((held_below, held_above)):

        @pl.when(has_last[way])
        def _(way=way):
            passes[way].wait_recv()

        def smooth_rows(a, way=way, kept=kept):
            for cols in columns:
                value = own_range(along_y, way * 3 + a, cols) + dot(back[a], kept[:, cols])
                fine[way * 3 + a, :, cols] = value.astype(bf16).astype(f32)

        loop(3, smooth_rows)

    for rim in hat_rims:
        rim.wait_recv()
    fill_edges(hat_edge_in, u)

    def coarse_tile(i):
        row = pl.multiple_of(i * 8, 8)
        here = pl.ds(row, 8)
        root, parts = strain_rows(u, [fine[3 + a, here] - fine[a, here] for a in range(3)], row)
        root = 2.0 * root
        for p in range(6):
            coarse[p, here] = root * parts[p]

    loop(depth // 8, coarse_tile)

    for rim in rims:
        rim.wait_recv()
    fill_edges(edge_in, v)

    def chunk(c):
        arrived(1, c)
        base = pl.multiple_of(c * quarter, quarter)

        def strain_tile(i):
            row = pl.multiple_of(base + i * 16, 16)
            here = pl.ds(row, 16)
            slopes_y = []
            for a in range(3):
                lower, upper = [
                    halo_in[way, 0, a, here].astype(f32) + halo_in[way, 1, a, here].astype(f32)
                    for way in range(2)
                ]
                slopes_y.append(upper - lower)
            scaled = [[] for _ in index_pairs]
            for top in (0, 8):
                root, parts = strain_rows(v, [s[top : top + 8] for s in slopes_y], row + top)
                magnitude = 0.5 * root
                nu[pl.ds(row + top, 8)] = magnitude
                for p, part in enumerate(parts):
                    scaled[p].append(magnitude * part)
            for p, halves in enumerate(scaled):
                rows = pl.ds(pl.multiple_of(p * quarter + i * 16, 16), 16)
                x[rows] = jnp.concatenate(halves, axis=0).astype(bf16)

        loop(quarter // 16, strain_tile)
        for cols in columns:
            value = dot(x[0 : 6 * quarter], table[:, cols]).astype(bf16)
            for p in range(6):
                rows = pl.ds(pl.multiple_of(p * depth + base, quarter), quarter)
                along_s[rows, cols] = value[p * quarter : (p + 1) * quarter]

    loop(chunks, chunk)
    out_s = [cross(along_s, 0, 3), cross(along_s, 1, 4)]

    def near_part(p):
        for cols in columns:
            fine[p, :, cols] = own_range(along_s, p, cols)

    loop(6, near_part)
    for copy in out_p:
        copy.wait_recv()
    for p, (a, b) in enumerate(index_pairs):
        for cols in columns:
            value = own_range(along, p, cols) + dot(back[p % 3], held[1 + p // 3, :, cols])
            here = slice(8, 8 + depth)
            leonard[p, :, cols] = value.astype(bf16).astype(f32) - u[a, here, cols] * u[b, here, cols]

    sums[...] = jnp.zeros_like(sums)
    for p in range(6):
        if p % 3 == 0:
            for copy in out_s[p // 3]:
                copy.wait_recv()
        for cols in columns:
            value = fine[p, :, cols] + dot(back[p % 3], held[3 + p // 3, :, cols])
            model = value.astype(bf16).astype(f32) - coarse[p, :, cols]
            for i, value in enumerate((leonard[p, :, cols] * model, model * model)):
                value = jnp.sum(value.reshape(depth // 8, 8, tile), axis=0)
                sums[i, :, cols] += pair_weights[p] * value

    for i in range(2):
        value = sums[i]
        part = value[:, 0:128]
        for left in range(128, nx, 128):
            part = part + value[:, left : left + 128]
        sums_out[i] = part
    shares = [
        remote(sums_out, sums_in.at[s - 1], sum_send.at[s - 1], sum_recv.at[s - 1], pz=ring(s))
        for s in range(1, n)
    ]
    for share in shares:
        share.start()
    total = sums_out[...]
    for s, share in enumerate(shares):
        share.wait_recv()
        total = total + sums_in[s]
    cells = float(nx * depth * n)
    mean = jnp.sum(jnp.sum(total, axis=2, keepdims=True), axis=1, keepdims=True) / cells
    coefficient = jnp.broadcast_to(mean[0] / (2.0 * (mean[1] + epsilon)), (8, nx))

    def scale(i):
        here = pl.ds(pl.multiple_of(i * 8, 8), 8)
        nu[here] = nu[here] * coefficient

    loop(depth // 8, scale)

    for turn in turns:
        turn.wait_recv()
    for copy in rims + hat_rims + out_v + out_p + out_s[0] + out_s[1] + turns + shares:
        copy.wait_send()
    for way in range(2):

        @pl.when(has_next[way])
        def _(way=way):
            passes[way].wait_send()
            for part, c in pieces:
                halo(way, part, c, 0).wait_send()
                halo(way, part, c, 1).wait_send()

        if detours:

            @pl.when(relay[way])
            def _(way=way):
                for part, c in pieces:
                    onward(way, part, c).wait_send()


def plane_body(velocity):
    n, ny = lax.axis_size("pz"), lax.axis_size("py")
    depth, nx = velocity.shape[2:]
    nz, width = depth * n, nx // n
    chunks = 8
    quarter = depth // chunks
    down, back, spans = cross_tables(
        {s: cross_factors(nz, depth, s) for s in (1, n - 1, 2)}, 3, depth
    )
    cells = np.arange(depth)
    near = filter_taps(nz)[(cells[:, None] - cells[None, :]) % nz]
    near = jnp.asarray(near, dtype=jnp.float32).astype(jnp.bfloat16)
    tables = (filter_table(nx), near, down, back)
    f32, bf16 = jnp.float32, jnp.bfloat16
    vmem, anywhere = pl.BlockSpec(memory_space=pltpu.VMEM), pl.BlockSpec(memory_space=pl.ANY)
    dma = pltpu.SemaphoreType.DMA
    rows = down.shape[0]
    scratch = [pltpu.VMEM(t.shape, bf16) for t in tables]
    scratch += [
        pltpu.VMEM((3, depth + 16, nx), f32),
        pltpu.VMEM((2, 3, depth, nx), bf16),
        pltpu.VMEM((2, 2, 3, depth, nx), bf16),
        pltpu.VMEM((2, 3, depth // 2, nx), bf16),
        pltpu.VMEM((3, depth + 16, nx), f32),
        pltpu.VMEM((3, depth, nx), bf16),
        pltpu.VMEM((3 * depth, nx), bf16),
        pltpu.VMEM((6 * depth, nx), bf16),
        pltpu.VMEM((6 * depth, nx), bf16),
        pltpu.VMEM((6 * depth, nx), bf16),
        pltpu.VMEM((max(depth, 6 * quarter), nx), bf16),
        pltpu.VMEM((6, depth, nx), f32),
        pltpu.VMEM((6, depth, nx), f32),
        pltpu.VMEM((6, depth, nx), f32),
    ]
    scratch += [pltpu.VMEM((2, 8, nx), f32)] * 4
    scratch += [pltpu.VMEM((5, rows, nx), bf16)] * 2 + [pltpu.VMEM((rows, nx), bf16)] * 2
    scratch += [
        pltpu.VMEM((2, 8, nx), f32),
        pltpu.VMEM((2, 8, 128), f32),
        pltpu.VMEM((n - 1, 2, 8, 128), f32),
    ]
    scratch += [dma((7,)), dma((2, 2)), dma((2, 2)), dma((2, 2, chunks, 2))]
    scratch += [dma((2, 2, chunks, 2))]
    scratch += [dma((2, chunks)), dma((2, chunks)), dma((5, n - 1)), dma((5, n - 1))]
    scratch += [dma((n - 1,))] * 2 + [dma((2,))] * 2 + [dma((n - 1,))] * 2
    nu_t, hat = pl.pallas_call(
        functools.partial(plane_kernel, n, ny, chunks, spans),
        in_specs=[anywhere] * 5,
        out_specs=[vmem, vmem],
        out_shape=[
            jax.ShapeDtypeStruct((depth, nx), f32),
            jax.ShapeDtypeStruct((3, nz, width), bf16),
        ],
        scratch_shapes=scratch,
        compiler_params=pltpu.CompilerParams(
            collective_id=0, has_side_effects=True, vmem_limit_bytes=60 * 1024 * 1024
        ),
    )(velocity[:, 0], *tables)
    return nu_t[None], hat[:, None]


def solution(mesh):
    in_specs = (P(None, "py", "pz", None),)
    out_specs = (P("py", "pz", None), P(None, "py", None, "pz"))

    def step(velocity):
        depth, nx = velocity.shape[2:]
        banded = mesh.shape["pz"] == 4 and depth % 128 == 0 and nx % 512 == 0
        return plane_body(velocity) if banded else body(velocity)

    return jax.shard_map(step, mesh=mesh, in_specs=in_specs, out_specs=out_specs, check_vma=False)
```
